128 devices in a mesh: batch: 4 (over z), seq: 16 (over y, x_lo, core), head: 2 (over x_hi).
Axes of the slice: x: 4 (x_hi: 2, x_lo: 2; x = x_hi * 2 + x_lo), y: 4, z: 4, core: 2. Of those that a mesh axis runs over, the one named last changes fastest.
Arguments:
- image_hidden: bfloat16 [8, 4096, 3072], P('batch', 'seq', 'head'), parts along dimension 0, may hold values from -6 to 6
- modulation: float32 [8, 3, 3072], P('batch'), parts along dimension 0, may hold values from -4 to 4
- qkv_weight: bfloat16 [3072, 3, 1536], P(None, None, 'head'), may hold values from -0.109375 to 0.109375
- out_weight: bfloat16 [1536, 3072], P('head'), may hold values from -0.15625 to 0.15625
- q_gain: float32 [128], replicated, may hold values from 1.2 to 2.5
- k_gain: float32 [128], replicated, may hold values from 1.2 to 2.5
- text_keys: bfloat16 [8, 512, 1536], P('batch', 'seq', 'head'), parts along dimension 0, may hold values from -10 to 10
- text_values: bfloat16 [8, 512, 1536], P('batch', 'seq', 'head'), parts along dimension 0, may hold values from -6 to 6
- stale_keys: bfloat16 [8, 4096, 1536], P('batch', 'seq', 'head'), parts along dimension 0, may hold values from -64 to 64
- stale_values: bfloat16 [8, 4096, 1536], P('batch', 'seq', 'head'), parts along dimension 0, may hold values from -6 to 6
- cached_residual: bfloat16 [8, 4096, 3072], P('batch', 'seq', 'head'), parts along dimension 0, may hold values from -6 to 6
- patch_of: int32 [64], P('batch'), parts along dimension 0, may hold values from 0 to 15, each once
- refresh: int32 [64], P('batch'), parts along dimension 0, may hold values from 0 to 1, as said below
- text_len: int32 [8], P('batch'), parts along dimension 0, may hold values from 64 to 512
Outputs:
- image_out: bfloat16 [8, 4096, 3072], P('batch', 'seq', 'head'), parts along dimension 0
The draws below stay inside these ranges and needn't reach their ends.
There are 4 independent parts, one for each index of `batch`. The reference program is written for one: setup_inputs(seed, part) draws one part's arguments, and reference() takes and returns one part's arrays. A program takes and returns all parts, laid end to end along the dimension named above; an argument that names none is the same for every part. Nothing has to cross between parts.
Inputs may be any that keep to these rules, and one draw needn't show every extreme that they name: `patch_of`: A permutation: every image band sits on exactly one index of seq. `refresh`: exactly 4 entries are 1, the rest 0.
All inputs are finite; a program needn't handle non-finite values.
Results may differ from the reference program's by a relative error of at most 0.012.
The reference program's roundings to bfloat16 on the way count: a program that leaves them out, or rounds other values in their place, can miss the bound.
Values may be sent and summed in bfloat16 or wider, within the bound.
No kernel may reach another device: no remote copies, remote signals or barrier semaphores. Data moves between devices by JAX's collectives and lax.ppermute only.
A program may use at most 192 MiB of HBM per device.

```python
import math
import jax
import jax.numpy as jnp
from jax import lax

D = 3072
HEADS = 12
HEAD_DIM = 128
GRID_W = 64
PROMPTS = 2
IMG_DEV = 256
IMG = 4096
TXT = 512
REFRESH = 4
N_SEQ = 16


def draw_stale_keys(key, part):
    shape = (PROMPTS, IMG, HEADS * HEAD_DIM)
    drawn = 1.8 * jax.random.truncated_normal(key, -5.0, 5.0, shape, jnp.float32)
    return drawn.astype(jnp.bfloat16)


def draw_refresh(key, part):
    shuffled = jax.random.permutation(key, N_SEQ)
    return (shuffled < REFRESH).astype(jnp.int32)


def steps_of(rng, shape, cuts, low, top_value):
    factor_of, own = 1.0, jax.random.fold_in(rng, 6)
    for dim, parts in cuts:
        heights = jnp.exp(jax.random.uniform(jax.random.fold_in(own, dim), (parts,), jnp.float32, low / len(cuts), top_value / len(cuts)))
        factor_of = factor_of * jnp.repeat(heights, shape[dim] // parts).reshape([-1 if axis == dim else 1 for axis in range(len(shape))])
    return factor_of


def bell_draw(own_key, extent, spread, limit, cuts=(), kind=jnp.bfloat16):
    level = steps_of(own_key, extent, cuts, -0.22, 0.18) if cuts else 1.0
    entries = jax.random.normal(own_key, extent, jnp.float32) * spread * level
    return jnp.minimum(jnp.maximum(entries, -limit), limit).astype(kind)


def setup_inputs(seed: int = 0, part: int = 0) -> dict:
    key_list = jax.random.split(jax.random.key(seed), 15)
    part_keys = jax.random.split(jax.random.fold_in(key_list[14], part), 15)
    image_hidden = bell_draw(part_keys[0], (PROMPTS, IMG, D), 1.0, 6.0, ((1, 16), (2, 2)))
    modulation = bell_draw(part_keys[1], (PROMPTS, 3, D), 0.8, 4.0, (), jnp.float32)
    qkv_weight = bell_draw(key_list[2], (D, 3, HEADS * HEAD_DIM), D ** -0.5, 0.109375, ((2, 2),))
    out_weight = bell_draw(key_list[3], (HEADS * HEAD_DIM, D), (HEADS * HEAD_DIM) ** -0.5, 0.15625, ((0, 2),))
    q_gain = jnp.clip(jnp.exp(jax.random.uniform(key_list[4], (HEAD_DIM,), jnp.float32, math.log(1.2), math.log(2.5))), 1.2, 2.5)
    k_gain = jnp.clip(jnp.exp(jax.random.uniform(key_list[5], (HEAD_DIM,), jnp.float32, math.log(1.2), math.log(2.5))), 1.2, 2.5)
    text_keys = bell_draw(part_keys[6], (PROMPTS, TXT, HEADS * HEAD_DIM), 1.8, 10.0, ((1, 16), (2, 2)))
    text_values = bell_draw(part_keys[7], (PROMPTS, TXT, HEADS * HEAD_DIM), 1.0, 6.0, ((1, 16), (2, 2)))
    stale_keys = draw_stale_keys(jax.random.fold_in(jax.random.fold_in(key_list[14], part), 71), part)
    stale_values = bell_draw(part_keys[9], (PROMPTS, IMG, HEADS * HEAD_DIM), 1.0, 6.0, ((1, 16), (2, 2)))
    cached_residual = bell_draw(part_keys[10], (PROMPTS, IMG, D), 1.0, 6.0, ((1, 16), (2, 2)))
    patch_of = jax.random.permutation(part_keys[11], N_SEQ).astype(jnp.int32)
    refresh = draw_refresh(jax.random.fold_in(jax.random.fold_in(key_list[14], part), 71), part)
    text_len = jax.random.randint(part_keys[13], (PROMPTS,), TXT // 8, TXT + 1).astype(jnp.int32)
    return dict(image_hidden=image_hidden, modulation=modulation, qkv_weight=qkv_weight, out_weight=out_weight, q_gain=q_gain, k_gain=k_gain, text_keys=text_keys, text_values=text_values, stale_keys=stale_keys, stale_values=stale_values, cached_residual=cached_residual, patch_of=patch_of, refresh=refresh, text_len=text_len)


epsilon = 1e-06

def rotary_tables(raster, head_dim, grid_width):
    half_dim = head_dim // 2
    first_pairs = head_dim // 16
    axis_pairs = (half_dim - first_pairs) // 2
    pair_index = jnp.arange(half_dim, dtype=jnp.int32)
    pair_local = jnp.where(pair_index < first_pairs + axis_pairs, pair_index - first_pairs, pair_index - first_pairs - axis_pairs)
    exponent = -pair_local.astype(jnp.float32) / float(axis_pairs)
    frequency = jnp.where(pair_index < first_pairs, jnp.float32(0.0), jnp.power(jnp.float32(10000.0), exponent))
    row_pos = (raster // grid_width).astype(jnp.float32)
    col_pos = (raster % grid_width).astype(jnp.float32)
    position = jnp.where(pair_index[None, :] < first_pairs + axis_pairs, row_pos[:, None], col_pos[:, None])
    angles = position * frequency[None, :]
    cosine = jnp.cos(angles)
    sine = jnp.sin(angles)
    return (jnp.concatenate([cosine, cosine], axis=-1), jnp.concatenate([-sine, sine], axis=-1))

def rms_rotate(vectors, gain_vec, cos_full, sin_full):
    scaled = vectors * lax.rsqrt(lax.optimization_barrier(jnp.mean(vectors * vectors, axis=-1, keepdims=True)) + epsilon) * gain_vec
    half_dim = vectors.shape[-1] // 2
    return scaled * cos_full[:, None, :] + jnp.roll(scaled, half_dim, axis=-1) * sin_full[:, None, :]

def reference(image_hidden, modulation, qkv_weight, out_weight, q_gain, k_gain, text_keys, text_values, stale_keys, stale_values, cached_residual, patch_of, refresh, text_len):
    channels = HEADS * HEAD_DIM
    hidden_f32 = image_hidden.astype(jnp.float32)
    row_mean = lax.optimization_barrier(jnp.mean(hidden_f32, axis=-1, keepdims=True))
    centered = hidden_f32 - row_mean
    variance = lax.optimization_barrier(jnp.mean(centered * centered, axis=-1, keepdims=True))
    normed = centered * lax.rsqrt(variance + epsilon)
    modulated = (normed * (1.0 + modulation[:, 1][:, None, :]) + modulation[:, 0][:, None, :]).astype(jnp.bfloat16)
    position = jnp.arange(IMG, dtype=jnp.int32)
    owner_seat = position // IMG_DEV
    raster = patch_of[owner_seat] * IMG_DEV + position % IMG_DEV
    cos_full, sin_full = rotary_tables(raster, HEAD_DIM, GRID_W)
    refreshed = refresh[owner_seat] == 1
    score_scale = HEAD_DIM ** (-0.5)
    results = []
    for prompt in range(PROMPTS):
        projected = jnp.dot(modulated[prompt], qkv_weight.reshape(D, 3 * channels), preferred_element_type=jnp.float32)
        projected = projected.reshape(IMG, 3, HEADS, HEAD_DIM)
        fresh_q = rms_rotate(projected[:, 0], q_gain, cos_full, sin_full).astype(jnp.bfloat16)
        fresh_k = rms_rotate(projected[:, 1], k_gain, cos_full, sin_full).astype(jnp.bfloat16)
        fresh_v = projected[:, 2].astype(jnp.bfloat16)
        stale_k = stale_keys[prompt].reshape(IMG, HEADS, HEAD_DIM)
        stale_v = stale_values[prompt].reshape(IMG, HEADS, HEAD_DIM)
        text_key_rows = text_keys[prompt].reshape(TXT, HEADS, HEAD_DIM)
        text_value_rows = text_values[prompt].reshape(TXT, HEADS, HEAD_DIM)
        key_mask = jnp.concatenate([jnp.arange(TXT, dtype=jnp.int32) < text_len[prompt], jnp.ones((IMG,), jnp.bool_)])

        def attend(seq_index):
            use_fresh = refreshed | (owner_seat == seq_index)
            key_rows = jnp.where(use_fresh[:, None, None], fresh_k, stale_k)
            value_rows = jnp.where(use_fresh[:, None, None], fresh_v, stale_v)
            all_keys = jnp.concatenate([text_key_rows, key_rows], axis=0)
            all_values = jnp.concatenate([text_value_rows, value_rows], axis=0)
            queries = lax.dynamic_slice_in_dim(fresh_q, seq_index * IMG_DEV, IMG_DEV, 0)
            scores = jnp.einsum('qhd,khd->hqk', queries.astype(jnp.float32), all_keys.astype(jnp.float32)) * score_scale
            scores = jnp.where(key_mask[None, None, :], scores, -1e+30)
            row_top = lax.optimization_barrier(jnp.max(scores, axis=-1, keepdims=True))
            weights = jnp.exp(scores - row_top)
            row_sums = lax.optimization_barrier(jnp.sum(weights, axis=-1))
            probs = weights.astype(jnp.bfloat16)
            numerator = jnp.einsum('hqk,khd->qhd', probs.astype(jnp.float32), all_values.astype(jnp.float32))
            return (numerator / jnp.transpose(row_sums)[:, :, None]).astype(jnp.bfloat16)
        attended = lax.map(attend, jnp.arange(N_SEQ, dtype=jnp.int32)).reshape(IMG, channels)
        projection = jnp.dot(attended, out_weight, preferred_element_type=jnp.float32)
        combined = hidden_f32[prompt] + modulation[prompt, 2][None, :] * projection + cached_residual[prompt].astype(jnp.float32)
        results.append(combined.astype(jnp.bfloat16))
    return jnp.stack(results, axis=0)
```

```python
import functools

import jax
import jax.numpy as jnp
from jax import lax
from jax.experimental import pallas as pl
from jax.experimental.pallas import tpu as pltpu
from jax.sharding import PartitionSpec as P

GRID_W = 64
EPS = 1e-06
LOG2E = 1.4426950408889634
F32 = jnp.float32
BF16 = jnp.bfloat16
NEG = -1e30
VMEM = 56 * 1024 * 1024
SLOTS = 8


def rotary_tables(raster, head_dim, grid_width):
    half_dim = head_dim // 2
    first_pairs = head_dim // 16
    axis_pairs = (half_dim - first_pairs) // 2
    pair_index = jnp.arange(half_dim, dtype=jnp.int32)
    pair_local = jnp.where(
        pair_index < first_pairs + axis_pairs,
        pair_index - first_pairs,
        pair_index - first_pairs - axis_pairs,
    )
    exponent = -pair_local.astype(F32) / float(axis_pairs)
    frequency = jnp.where(pair_index < first_pairs, F32(0.0), jnp.power(F32(10000.0), exponent))
    row_pos = (raster // grid_width).astype(F32)
    col_pos = (raster % grid_width).astype(F32)
    position = jnp.where(
        pair_index[None, :] < first_pairs + axis_pairs, row_pos[:, None], col_pos[:, None]
    )
    angles = position * frequency[None, :]
    cosine = jnp.cos(angles)
    sine = jnp.sin(angles)
    return (jnp.concatenate([cosine, cosine], axis=-1), jnp.concatenate([-sine, sine], axis=-1))


def qkv_body(
    info, own, oth, mod_own, mod_oth, w_own, w_oth, gains, cos, sin, stale_k, stale_v, send, fresh, mod_s
):
    n = pl.program_id(0)
    prompts, rows, part = own.shape
    width = 2 * part
    tile = 16

    @pl.when(n == 0)
    def _():
        for p in range(prompts):
            def norm(i, c):
                at = pl.multiple_of(i * tile, tile)
                a = own[p, pl.ds(at, tile), :].astype(F32)
                b = oth[p, pl.ds(at, tile), :].astype(F32)
                mean = (jnp.sum(a, -1, keepdims=True) + jnp.sum(b, -1, keepdims=True)) / width
                a, b = a - mean, b - mean
                var = (jnp.sum(a * a, -1, keepdims=True) + jnp.sum(b * b, -1, keepdims=True)) / width
                inv = lax.rsqrt(var + EPS)
                a = a * inv * (1.0 + mod_own[p, 1:2, :]) + mod_own[p, 0:1, :]
                b = b * inv * (1.0 + mod_oth[p, 1:2, :]) + mod_oth[p, 0:1, :]
                to = pl.multiple_of(p * rows + i * tile, tile)
                mod_s[pl.ds(to, tile), 0:part] = a.astype(BF16)
                mod_s[pl.ds(to, tile), part:width] = b.astype(BF16)
                return c

            lax.fori_loop(0, rows // tile, norm, 0)

    acc = jnp.dot(mod_s[:, 0:part], w_own[...], preferred_element_type=F32)
    acc = acc + jnp.dot(mod_s[:, part:width], w_oth[...], preferred_element_type=F32)
    per_kind = pl.num_programs(0) // 3
    heads = acc.shape[1] // 128
    flag = info[1]

    def turned(x, gain):
        x = x * lax.rsqrt(jnp.mean(x * x, axis=-1, keepdims=True) + EPS) * gain
        return x * cos[...] + pltpu.roll(x, 64, 1) * sin[...]

    def piece(p, e):
        return acc[p * rows : (p + 1) * rows, e * 128 : (e + 1) * 128]

    @pl.when(n < per_kind)
    def _():
        for p in range(prompts):
            for e in range(heads):
                send[p, e, 0] = turned(piece(p, e), gains[0:1, :]).astype(BF16)

    @pl.when((n >= per_kind) & (n < 2 * per_kind))
    def _():
        for p in range(prompts):
            for e in range(heads):
                new = turned(piece(p, e), gains[1:2, :]).astype(BF16)
                fresh[p, e, 0] = new
                send[p, e, 0] = jnp.where(flag == 1, new, stale_k[p, :, e * 128 : (e + 1) * 128])

    @pl.when(n >= 2 * per_kind)
    def _():
        for p in range(prompts):
            for e in range(heads):
                new = piece(p, e).astype(BF16)
                fresh[p, e, 0] = new
                send[p, e, 0] = jnp.where(flag == 1, new, stale_v[p, :, e * 128 : (e + 1) * 128])


def qkv(info, own, oth, modulation, w, gains, cos, sin, stale_k, stale_v):
    prompts, rows, part = own.shape
    channels = stale_k.shape[2]
    heads = channels // 128
    per = 2
    kind = heads // per
    steps = 3 * kind
    bn = per * 128
    whole = lambda *shape: pl.BlockSpec(shape, lambda n, s: (0,) * len(shape))
    return pl.pallas_call(
        qkv_body,
        grid_spec=pltpu.PrefetchScalarGridSpec(
            num_scalar_prefetch=1,
            grid=(steps,),
            in_specs=[
                whole(prompts, rows, part),
                whole(prompts, rows, part),
                pl.BlockSpec((prompts, 3, part), lambda n, s: (0, 0, s[0])),
                pl.BlockSpec((prompts, 3, part), lambda n, s: (0, 0, 1 - s[0])),
                pl.BlockSpec((part, bn), lambda n, s: (s[0], n)),
                pl.BlockSpec((part, bn), lambda n, s: (1 - s[0], n)),
                whole(2, 128),
                whole(rows, 128),
                whole(rows, 128),
                pl.BlockSpec((prompts, rows, bn), lambda n, s: (0, 0, jnp.clip(n - kind, 0, kind - 1))),
                pl.BlockSpec((prompts, rows, bn), lambda n, s: (0, 0, jnp.clip(n - 2 * kind, 0, kind - 1))),
            ],
            out_specs=[
                pl.BlockSpec((prompts, per, 1, rows, 128), lambda n, s: (0, n % kind, n // kind, 0, 0)),
                pl.BlockSpec(
                    (prompts, per, 1, rows, 128),
                    lambda n, s: (0, jnp.maximum(n - kind, 0) % kind, jnp.maximum(n - kind, 0) // kind, 0, 0),
                ),
            ],
            scratch_shapes=[pltpu.VMEM((prompts * rows, 2 * part), BF16)],
        ),
        out_shape=[
            jax.ShapeDtypeStruct((prompts, SLOTS, 3, rows, 128), BF16),
            jax.ShapeDtypeStruct((prompts, heads, 2, rows, 128), BF16),
        ],
        compiler_params=pltpu.CompilerParams(
            dimension_semantics=("arbitrary",), vmem_limit_bytes=VMEM
        ),
        cost_estimate=pl.CostEstimate(
            flops=2 * prompts * rows * 2 * part * steps * bn, bytes_accessed=20_000_000, transcendentals=0
        ),
        name="qkv",
    )(info, own, oth, modulation, modulation, w, w, gains, cos, sin, stale_k, stale_v)


def diag_body(q, kv, out, lse):
    c = 128**-0.5 * LOG2E
    for e in range(q.shape[1]):
        s = lax.dot_general(q[0, e, 0], kv[0, e, 0], (((1,), (1,)), ((), ())), preferred_element_type=F32) * c
        top = jnp.max(s, axis=-1, keepdims=True)
        w = jnp.exp2(s - top)
        total = jnp.sum(w, axis=-1, keepdims=True)
        o = jnp.dot(w.astype(BF16), kv[0, e, 1], preferred_element_type=F32)
        out[0, e] = (o / total).astype(BF16)
        wide = jnp.broadcast_to(top + jnp.log2(total), (q.shape[3], 128))
        lse[0, e] = jnp.transpose(wide)[0:8, :]


def diag(send, fresh):
    prompts, heads, _, rows, _ = fresh.shape
    per = 2
    return pl.pallas_call(
        diag_body,
        grid=(prompts, heads // per),
        in_specs=[
            pl.BlockSpec((1, per, 1, rows, 128), lambda p, j: (p, j, 0, 0, 0)),
            pl.BlockSpec((1, per, 2, rows, 128), lambda p, j: (p, j, 0, 0, 0)),
        ],
        out_specs=[
            pl.BlockSpec((1, per, rows, 128), lambda p, j: (p, j, 0, 0)),
            pl.BlockSpec((1, per, 8, rows), lambda p, j: (p, j, 0, 0)),
        ],
        out_shape=[
            jax.ShapeDtypeStruct((prompts, SLOTS, rows, 128), BF16),
            jax.ShapeDtypeStruct((prompts, SLOTS, 8, rows), F32),
        ],
        compiler_params=pltpu.CompilerParams(
            dimension_semantics=("arbitrary", "arbitrary"), vmem_limit_bytes=VMEM
        ),
        cost_estimate=pl.CostEstimate(
            flops=4 * prompts * heads * rows * rows * 128, bytes_accessed=4_000_000, transcendentals=prompts * heads * rows * rows
        ),
        name="diag",
    )(send, fresh)


def attend_body(info, got, text, out, stat, s_ref):
    b = pl.program_id(0)
    blocks, _, rows, _ = got.shape
    c = 128**-0.5 * LOG2E
    q = got[b, 0]
    txt = text.shape[1]
    tiles = txt // rows + blocks - 1
    contract = (((1,), (1,)), ((), ()))

    def keys(i, which):
        if i < txt // rows:
            return text[which, i * rows : (i + 1) * rows, :]
        return got[lax.rem(b + 1 + (i - txt // rows), blocks), 1 + which]

    top = None
    for i in range(tiles):
        s = lax.dot_general(q, keys(i, 0), contract, preferred_element_type=F32)
        if i < txt // rows:
            at = i * rows + lax.broadcasted_iota(jnp.int32, s.shape, 1)
            s = jnp.where(at < info[0], s, NEG)
        s_ref[i] = s
        for e in range(rows // 128):
            part = s[:, e * 128 : (e + 1) * 128]
            top = part if top is None else jnp.maximum(top, part)
    top = jnp.max(top, axis=-1, keepdims=True) * c
    total = None
    acc = None
    for i in range(tiles):
        w = jnp.exp2(s_ref[i] * c - top)
        for e in range(rows // 128):
            part = w[:, e * 128 : (e + 1) * 128]
            total = part if total is None else total + part
        o = jnp.dot(w.astype(BF16), keys(i, 1), preferred_element_type=F32)
        acc = o if acc is None else acc + o
    total = jnp.sum(total, axis=-1, keepdims=True)
    out[0] = acc
    lane = lax.broadcasted_iota(jnp.int32, (rows, 128), 1)
    stat[0] = jnp.where(lane < 64, top, total)


def attend(info, got, text):
    blocks, _, rows, _ = got.shape
    txt = text.shape[1]
    tiles = txt // rows + blocks - 1
    return pl.pallas_call(
        attend_body,
        grid_spec=pltpu.PrefetchScalarGridSpec(
            num_scalar_prefetch=1,
            grid=(blocks,),
            in_specs=[
                pl.BlockSpec(got.shape, lambda b, s: (0, 0, 0, 0)),
                pl.BlockSpec(text.shape, lambda b, s: (0, 0, 0)),
            ],
            out_specs=[
                pl.BlockSpec((1, rows, 128), lambda b, s: (b, 0, 0)),
                pl.BlockSpec((1, rows, 128), lambda b, s: (b, 0, 0)),
            ],
            scratch_shapes=[pltpu.VMEM((tiles, rows, rows), F32)],
        ),
        out_shape=[
            jax.ShapeDtypeStruct((blocks, rows, 128), F32),
            jax.ShapeDtypeStruct((blocks, rows, 128), F32),
        ],
        compiler_params=pltpu.CompilerParams(
            dimension_semantics=("arbitrary",), vmem_limit_bytes=VMEM
        ),
        cost_estimate=pl.CostEstimate(
            flops=4 * blocks * rows * tiles * rows * 128 * 2,
            bytes_accessed=8_000_000,
            transcendentals=blocks * rows * tiles * rows,
        ),
        name="attend",
    )(info, got, text)


def join_body(acc, stat, own, lse, out):
    rows = acc.shape[1]
    for e in range(acc.shape[0]):
        top = stat[e, :, 0:1]
        total = stat[e, :, 64:65]
        other = jnp.transpose(jnp.broadcast_to(lse[e, 0:1, :], (128, rows)))
        high = jnp.maximum(other, top)
        u = jnp.exp2(top - high)
        w = jnp.exp2(other - high)
        o = (acc[e] * u + own[e].astype(F32) * w) / (total * u + w)
        o = o.astype(BF16)
        out[e, 0] = o
        out[e, 1] = o


def join(acc, stat, own, lse):
    blocks, rows, _ = acc.shape
    per = 4
    return pl.pallas_call(
        join_body,
        grid=(blocks // per,),
        in_specs=[
            pl.BlockSpec((per, rows, 128), lambda b: (b, 0, 0)),
            pl.BlockSpec((per, rows, 128), lambda b: (b, 0, 0)),
            pl.BlockSpec((per, rows, 128), lambda b: (b, 0, 0)),
            pl.BlockSpec((per, 8, rows), lambda b: (b, 0, 0)),
        ],
        out_specs=pl.BlockSpec((per, 2, rows, 128), lambda b: (b, 0, 0, 0)),
        out_shape=jax.ShapeDtypeStruct((blocks, 2, rows, 128), BF16),
        compiler_params=pltpu.CompilerParams(
            dimension_semantics=("arbitrary",), vmem_limit_bytes=VMEM
        ),
        name="join",
    )(acc, stat, own, lse)


def project_body(info, got, w_own, w_oth, gate, hidden, cached, out, all_s):
    n = pl.program_id(0)
    prompts, rows, _ = hidden.shape
    part = w_own.shape[0]
    heads = part // 128
    h = info[0]

    @pl.when(n == 0)
    def _():
        for p in range(prompts):
            for k in range(2):
                seat = h if k == 0 else 1 - h
                for j in range(heads):
                    all_s[p * rows : (p + 1) * rows, (k * heads + j) * 128 : (k * heads + j + 1) * 128] = got[
                        (p * SLOTS + j) * 2 + seat
                    ]

    acc = jnp.dot(all_s[:, 0:part], w_own[...], preferred_element_type=F32)
    acc = acc + jnp.dot(all_s[:, part : 2 * part], w_oth[...], preferred_element_type=F32)
    for p in range(prompts):
        y = hidden[p].astype(F32) + gate[p] * acc[p * rows : (p + 1) * rows, :]
        out[p] = (y + cached[p].astype(F32)).astype(BF16)


def project(info, got, w_out, w_oth, gate, hidden, cached):
    prompts, rows, width = hidden.shape
    part = w_out.shape[0]
    bn = 512
    steps = width // bn
    return pl.pallas_call(
        project_body,
        grid_spec=pltpu.PrefetchScalarGridSpec(
            num_scalar_prefetch=1,
            grid=(steps,),
            in_specs=[
                pl.BlockSpec(got.shape, lambda n, s: (0, 0, 0)),
                pl.BlockSpec((part, bn), lambda n, s: (0, s[0] * steps + n)),
                pl.BlockSpec((part, bn), lambda n, s: (0, n)),
                pl.BlockSpec((prompts, 1, bn), lambda n, s: (0, 0, n)),
                pl.BlockSpec((prompts, rows, bn), lambda n, s: (0, 0, n)),
                pl.BlockSpec((prompts, rows, bn), lambda n, s: (0, 0, n)),
            ],
            out_specs=pl.BlockSpec((prompts, rows, bn), lambda n, s: (0, 0, n)),
            scratch_shapes=[pltpu.VMEM((prompts * rows, 2 * part), BF16)],
        ),
        out_shape=jax.ShapeDtypeStruct((prompts, rows, width), BF16),
        compiler_params=pltpu.CompilerParams(
            dimension_semantics=("arbitrary",), vmem_limit_bytes=VMEM
        ),
        cost_estimate=pl.CostEstimate(
            flops=4 * prompts * rows * part * width, bytes_accessed=12_000_000, transcendentals=0
        ),
        name="project",
    )(info, got, w_out, w_oth, gate, hidden, cached)


def per_device(
    image_hidden,
    modulation,
    qkv_weight,
    out_weight,
    q_gain,
    k_gain,
    text_keys,
    text_values,
    stale_keys,
    stale_values,
    cached_residual,
    patch_of,
    refresh,
    text_len,
):
    prompts, rows, width_part = image_hidden.shape
    head_dim = q_gain.shape[0]
    channels = out_weight.shape[0]
    heads = channels // head_dim
    seat = lax.axis_index("seq")
    head_seat = lax.axis_index("head")
    batch_seat = lax.axis_index("batch")
    n_seq = lax.axis_size("seq")
    n_batch = lax.axis_size("batch")
    swap = [(0, 1), (1, 0)]

    other_hidden = lax.ppermute(image_hidden, "head", swap)

    text = jnp.stack([text_keys, text_values], 1)
    t_rows = text.shape[2]
    text = text.reshape(prompts, 2, t_rows, heads, head_dim).transpose(0, 3, 1, 2, 4)
    text = jnp.pad(text, ((0, 0), (0, SLOTS - heads), (0, 0), (0, 0), (0, 0)))
    text = text.reshape(n_seq, 2, t_rows, head_dim)
    text = lax.all_to_all(text, "seq", split_axis=0, concat_axis=0, tiled=True)
    text = text.transpose(1, 0, 2, 3).reshape(2, n_seq * t_rows, head_dim)

    seats = jnp.arange(n_seq, dtype=jnp.int32)
    own_band = jnp.sum(jnp.where(seats == seat, patch_of, 0))
    own_flag = jnp.sum(jnp.where(seats == seat, refresh, 0))
    raster = own_band * rows + jnp.arange(rows, dtype=jnp.int32)
    cos, sin = rotary_tables(raster, head_dim, GRID_W)
    info = jnp.stack([head_seat.astype(jnp.int32), own_flag.astype(jnp.int32)])
    weight = qkv_weight.reshape(2 * width_part, 3 * channels)
    send, fresh = qkv(
        info,
        image_hidden,
        other_hidden,
        modulation,
        weight,
        jnp.stack([q_gain, k_gain]),
        cos,
        sin,
        stale_keys,
        stale_values,
    )
    got = lax.all_to_all(
        send.reshape(n_seq, 3, rows, head_dim), "seq", split_axis=0, concat_axis=0, tiled=True
    )

    share = channels // n_batch
    piece = lax.dynamic_slice(
        out_weight, (batch_seat * share, (1 - head_seat) * width_part), (share, width_part)
    )
    piece, _ = lax.optimization_barrier((piece, other_hidden))
    piece = lax.ppermute(piece, "head", swap)
    w_oth = jnp.zeros((n_batch, share, width_part), BF16)
    w_oth = lax.dynamic_update_slice(w_oth, piece[None], (batch_seat, 0, 0))
    for d in range(1, n_batch):
        moved = lax.ppermute(piece, "batch", [(i, (i + d) % n_batch) for i in range(n_batch)])
        w_oth = lax.dynamic_update_slice(w_oth, moved[None], ((batch_seat - d) % n_batch, 0, 0))
    w_oth = w_oth.reshape(channels, width_part)

    own_part, own_lse = diag(send, fresh)
    unit_prompt = jnp.minimum(seat // SLOTS, prompts - 1)
    length = jnp.sum(jnp.where(jnp.arange(prompts) == unit_prompt, text_len, 0)).astype(jnp.int32)
    acc, stat = attend(length[None], got, text)
    own_part = lax.all_to_all(
        own_part.reshape(n_seq, rows, head_dim), "seq", split_axis=0, concat_axis=0, tiled=True
    )
    own_lse = lax.all_to_all(
        own_lse.reshape(n_seq, 8, rows), "seq", split_axis=0, concat_axis=0, tiled=True
    )
    back = join(acc, stat, own_part, own_lse)
    back = lax.all_to_all(
        back.reshape(n_seq * 2, rows, head_dim), ("seq", "head"), split_axis=0, concat_axis=0, tiled=True
    )
    gate = lax.dynamic_slice_in_dim(modulation[:, 2:3], head_seat * width_part, width_part, 2)
    return project(info, back, out_weight, w_oth, gate, image_hidden, cached_residual)


def solution(mesh):
    in_specs = (
        P("batch", "seq", "head"),
        P("batch", None, None),
        P(None, None, "head"),
        P("head", None),
        P(),
        P(),
        P("batch", "seq", "head"),
        P("batch", "seq", "head"),
        P("batch", "seq", "head"),
        P("batch", "seq", "head"),
        P("batch", "seq", "head"),
        P("batch"),
        P("batch"),
        P("batch"),
    )
    out_specs = P("batch", "seq", "head")
    return jax.shard_map(
        per_device, mesh=mesh, in_specs=in_specs, out_specs=out_specs, check_vma=False
    )
```

```python
import jax
import jax.numpy as jnp
from jax import lax
from jax.experimental import pallas as pl
from jax.experimental.pallas import tpu as pltpu
from jax.sharding import PartitionSpec as P


GRID_W = 64
EPS = 1e-06
LOG2E = 1.4426950408889634
F32 = jnp.float32
BF16 = jnp.bfloat16
NEG = -1e30
VMEM = 56 * 1024 * 1024
SLOTS = 8


def rotary_tables(raster, head_dim, grid_width):
    half_dim = head_dim // 2
    first_pairs = head_dim // 16
    axis_pairs = (half_dim - first_pairs) // 2
    pair_index = jnp.arange(half_dim, dtype=jnp.int32)
    pair_local = jnp.where(
        pair_index < first_pairs + axis_pairs,
        pair_index - first_pairs,
        pair_index - first_pairs - axis_pairs,
    )
    exponent = -pair_local.astype(F32) / float(axis_pairs)
    frequency = jnp.where(pair_index < first_pairs, F32(0.0), jnp.power(F32(10000.0), exponent))
    row_pos = (raster // grid_width).astype(F32)
    col_pos = (raster % grid_width).astype(F32)
    position = jnp.where(
        pair_index[None, :] < first_pairs + axis_pairs, row_pos[:, None], col_pos[:, None]
    )
    angles = position * frequency[None, :]
    cosine = jnp.cos(angles)
    sine = jnp.sin(angles)
    return (jnp.concatenate([cosine, cosine], axis=-1), jnp.concatenate([-sine, sine], axis=-1))


def qkv_body(
    info, own, oth, mod_own, mod_oth, w_own, w_oth, gains, cos, sin, stale_k, stale_v, send, fresh, mod_s
):
    n = pl.program_id(0)
    prompts, rows, part = own.shape
    width = 2 * part
    tile = 16

    @pl.when(n == 0)
    def _():
        for p in range(prompts):
            def norm(i, c):
                at = pl.multiple_of(i * tile, tile)
                a = own[p, pl.ds(at, tile), :].astype(F32)
                b = oth[p, pl.ds(at, tile), :].astype(F32)
                mean = (jnp.sum(a, -1, keepdims=True) + jnp.sum(b, -1, keepdims=True)) / width
                a, b = a - mean, b - mean
                var = (jnp.sum(a * a, -1, keepdims=True) + jnp.sum(b * b, -1, keepdims=True)) / width
                inv = lax.rsqrt(var + EPS)
                a = a * inv * (1.0 + mod_own[1, p : p + 1, :]) + mod_own[0, p : p + 1, :]
                b = b * inv * (1.0 + mod_oth[1, p : p + 1, :]) + mod_oth[0, p : p + 1, :]
                to = pl.multiple_of(p * rows + i * tile, tile)
                mod_s[pl.ds(to, tile), 0:part] = a.astype(BF16)
                mod_s[pl.ds(to, tile), part:width] = b.astype(BF16)
                return c

            lax.fori_loop(0, rows // tile, norm, 0, unroll=4)

    heads = w_own.shape[2] // 128
    per = 2
    flag = info[1]

    def products():
        for j in range(0, heads, per):
            cols = slice(j * 128, (j + per) * 128)
            acc = jnp.dot(mod_s[:, 0:part], w_own[0, :, cols], preferred_element_type=F32)
            acc = acc + jnp.dot(mod_s[:, part:width], w_oth[0, :, cols], preferred_element_type=F32)
            for p in range(prompts):
                for e in range(per):
                    yield p, j + e, acc[p * rows : (p + 1) * rows, e * 128 : (e + 1) * 128]

    def turned(x, gain):
        x = x * lax.rsqrt(jnp.mean(x * x, axis=-1, keepdims=True) + EPS) * gain
        return x * cos[...] + pltpu.roll(x, 64, 1) * sin[...]

    @pl.when(n == 0)
    def _():
        for p, j, x in products():
            send[p, j, 0] = turned(x, gains[0:1, :]).astype(BF16)

    @pl.when(n == 1)
    def _():
        for p, j, x in products():
            new = turned(x, gains[1:2, :]).astype(BF16)
            fresh[p, j, 0] = new
            send[p, j, 0] = jnp.where(flag == 1, new, stale_k[p, :, j * 128 : (j + 1) * 128])

    @pl.when(n == 2)
    def _():
        for p, j, x in products():
            new = x.astype(BF16)
            fresh[p, j, 0] = new
            send[p, j, 0] = jnp.where(flag == 1, new, stale_v[p, :, j * 128 : (j + 1) * 128])


def qkv(info, own, oth, modulation, w, gains, cos, sin, stale_k, stale_v):
    prompts, rows, part = own.shape
    channels = stale_k.shape[2]
    heads = channels // 128
    whole = lambda *shape: pl.BlockSpec(shape, lambda n, s: (0,) * len(shape))
    return pl.pallas_call(
        qkv_body,
        grid_spec=pltpu.PrefetchScalarGridSpec(
            num_scalar_prefetch=1,
            grid=(3,),
            in_specs=[
                whole(prompts, rows, part),
                whole(prompts, rows, part),
                pl.BlockSpec((3, prompts, part), lambda n, s: (0, 0, s[0])),
                pl.BlockSpec((3, prompts, part), lambda n, s: (0, 0, 1 - s[0])),
                pl.BlockSpec((1, part, channels), lambda n, s: (n, s[0], 0)),
                pl.BlockSpec((1, part, channels), lambda n, s: (n, 1 - s[0], 0)),
                whole(2, 128),
                whole(rows, 128),
                whole(rows, 128),
                whole(prompts, rows, channels),
                whole(prompts, rows, channels),
            ],
            out_specs=[
                pl.BlockSpec((prompts, SLOTS, 1, rows, 128), lambda n, s: (0, 0, n, 0, 0)),
                pl.BlockSpec(
                    (prompts, heads, 1, rows, 128), lambda n, s: (0, 0, jnp.maximum(n - 1, 0), 0, 0)
                ),
            ],
            scratch_shapes=[pltpu.VMEM((prompts * rows, 2 * part), BF16)],
        ),
        out_shape=[
            jax.ShapeDtypeStruct((prompts, SLOTS, 3, rows, 128), BF16),
            jax.ShapeDtypeStruct((prompts, heads, 2, rows, 128), BF16),
        ],
        compiler_params=pltpu.CompilerParams(
            dimension_semantics=("arbitrary",), vmem_limit_bytes=VMEM
        ),
        cost_estimate=pl.CostEstimate(
            flops=2 * prompts * rows * 2 * part * 3 * channels, bytes_accessed=20_000_000, transcendentals=0
        ),
        name="qkv",
    )(info, own, oth, modulation, modulation, w, w, gains, cos, sin, stale_k, stale_v)


def diag_body(q, kv, out):
    c = 128**-0.5 * LOG2E
    rows = q.shape[3]
    for e in range(q.shape[1]):
        s = lax.dot_general(q[0, e, 0], kv[0, e, 0], (((1,), (1,)), ((), ())), preferred_element_type=F32) * c
        top = jnp.max(s, axis=-1, keepdims=True)
        w = jnp.exp2(s - top)
        total = jnp.sum(w, axis=-1, keepdims=True)
        o = jnp.dot(w.astype(BF16), kv[0, e, 1], preferred_element_type=F32)
        out[0, e, 0:rows, :] = (o / total).astype(BF16)
        lse = jnp.transpose(jnp.broadcast_to(top + jnp.log2(total), (rows, 128)))[0:8, :]
        first = lse.astype(BF16).astype(F32)
        second = (lse - first).astype(BF16).astype(F32)
        third = lse - first - second
        at = lax.broadcasted_iota(jnp.int32, lse.shape, 0)
        pieces = jnp.where(at == 0, first, jnp.where(at == 1, second, third))
        pieces = jnp.concatenate([pieces[:, i : i + 128] for i in range(0, rows, 128)], 0)
        out[0, e, rows : rows + rows // 16, :] = pieces.astype(BF16)


def diag(send, fresh):
    prompts, heads, _, rows, _ = fresh.shape
    tall = rows + rows // 16
    per = heads
    return pl.pallas_call(
        diag_body,
        grid=(prompts,),
        in_specs=[
            pl.BlockSpec((1, per, 1, rows, 128), lambda p: (p, 0, 0, 0, 0)),
            pl.BlockSpec((1, per, 2, rows, 128), lambda p: (p, 0, 0, 0, 0)),
        ],
        out_specs=pl.BlockSpec((1, SLOTS, tall, 128), lambda p: (p, 0, 0, 0)),
        out_shape=jax.ShapeDtypeStruct((prompts, SLOTS, tall, 128), BF16),
        compiler_params=pltpu.CompilerParams(
            dimension_semantics=("arbitrary",), vmem_limit_bytes=VMEM
        ),
        cost_estimate=pl.CostEstimate(
            flops=4 * prompts * heads * rows * rows * 128,
            bytes_accessed=4_000_000,
            transcendentals=prompts * heads * rows * rows,
        ),
        name="diag",
    )(send, fresh)


def attend_body(info, got, text, out, stat, s_even, s_odd, top_s):
    g = pl.program_id(0)
    blocks, _, rows, _ = got.shape
    c = 128**-0.5 * LOG2E
    txt = text.shape[1]
    lead = txt // rows
    tiles = lead + blocks - 1
    contract = (((1,), (1,)), ((), ()))

    def keys(b, i, which):
        if i < lead:
            return text[which, i * rows : (i + 1) * rows, :]
        return got[lax.rem(b + 1 + (i - lead), blocks), 1 + which]

    def score(b, i, top, s_ref):
        s = lax.dot_general(got[b, 0], keys(b, i, 0), contract, preferred_element_type=F32)
        if i < lead:
            at = i * rows + lax.broadcasted_iota(jnp.int32, s.shape, 1)
            s = jnp.where(at < info[0], s, NEG)
        s_ref[i] = s
        for e in range(rows // 128):
            part = s[:, e * 128 : (e + 1) * 128]
            top = part if top is None else jnp.maximum(top, part)
        return top

    def lane_top(top):
        return jnp.broadcast_to(jnp.max(top, axis=-1, keepdims=True) * c, (rows, 128))

    @pl.when(g == 0)
    def _():
        top = None
        for i in range(tiles):
            top = score(0, i, top, s_even)
        top_s[...] = lane_top(top)

    top = top_s[...]
    for k in range(2):
        b = 2 * g + k
        nxt = lax.rem(b + 1, blocks)
        here, there = (s_even, s_odd) if k == 0 else (s_odd, s_even)
        total = None
        acc = None
        nxt_top = None
        for i in range(tiles):
            nxt_top = score(nxt, i, nxt_top, there)
            s = here[i]
            w = []
            for e in range(rows // 128):
                part = jnp.exp2(s[:, e * 128 : (e + 1) * 128] * c - top)
                total = part if total is None else total + part
                w.append(part.astype(BF16))
            o = jnp.dot(jnp.concatenate(w, 1), keys(b, i, 1), preferred_element_type=F32)
            acc = o if acc is None else acc + o
        total = jnp.sum(total, axis=-1, keepdims=True)
        out[k] = acc
        lane = lax.broadcasted_iota(jnp.int32, (rows, 128), 1)
        stat[k] = jnp.where(lane < 64, top, total)
        top = lane_top(nxt_top)
    top_s[...] = top


def attend(info, got, text):
    blocks, _, rows, _ = got.shape
    txt = text.shape[1]
    tiles = txt // rows + blocks - 1
    return pl.pallas_call(
        attend_body,
        grid_spec=pltpu.PrefetchScalarGridSpec(
            num_scalar_prefetch=1,
            grid=(blocks // 2,),
            in_specs=[
                pl.BlockSpec(got.shape, lambda b, s: (0, 0, 0, 0)),
                pl.BlockSpec(text.shape, lambda b, s: (0, 0, 0)),
            ],
            out_specs=[
                pl.BlockSpec((2, rows, 128), lambda b, s: (b, 0, 0)),
                pl.BlockSpec((2, rows, 128), lambda b, s: (b, 0, 0)),
            ],
            scratch_shapes=[
                pltpu.VMEM((tiles, rows, rows), F32),
                pltpu.VMEM((tiles, rows, rows), F32),
                pltpu.VMEM((rows, 128), F32),
            ],
        ),
        out_shape=[
            jax.ShapeDtypeStruct((blocks, rows, 128), F32),
            jax.ShapeDtypeStruct((blocks, rows, 128), F32),
        ],
        compiler_params=pltpu.CompilerParams(
            dimension_semantics=("arbitrary",), vmem_limit_bytes=VMEM
        ),
        cost_estimate=pl.CostEstimate(
            flops=4 * blocks * rows * tiles * rows * 128 * 2,
            bytes_accessed=8_000_000,
            transcendentals=blocks * rows * tiles * rows,
        ),
        name="attend",
    )(info, got, text)


def join_body(acc, stat, own, out):
    rows = acc.shape[1]
    for e in range(acc.shape[0]):
        top = stat[e, :, 0:1]
        total = stat[e, :, 64:65]
        pieces = own[e, rows : rows + rows // 16, :].astype(F32)
        other = []
        for i in range(0, rows // 16, 8):
            lse = pieces[i : i + 1] + pieces[i + 1 : i + 2] + pieces[i + 2 : i + 3]
            other.append(jnp.transpose(jnp.broadcast_to(lse, (128, 128))))
        other = jnp.concatenate(other, 0)
        high = jnp.maximum(other, top)
        u = jnp.exp2(top - high)
        w = jnp.exp2(other - high)
        o = (acc[e] * u + own[e, 0:rows, :].astype(F32) * w) / (total * u + w)
        o = o.astype(BF16)
        out[e, 0] = o
        out[e, 1] = o


def join(acc, stat, own):
    blocks, rows, _ = acc.shape
    per = 4
    return pl.pallas_call(
        join_body,
        grid=(blocks // per,),
        in_specs=[
            pl.BlockSpec((per, rows, 128), lambda b: (b, 0, 0)),
            pl.BlockSpec((per, rows, 128), lambda b: (b, 0, 0)),
            pl.BlockSpec((per, own.shape[1], 128), lambda b: (b, 0, 0)),
        ],
        out_specs=pl.BlockSpec((per, 2, rows, 128), lambda b: (b, 0, 0, 0)),
        out_shape=jax.ShapeDtypeStruct((blocks, 2, rows, 128), BF16),
        compiler_params=pltpu.CompilerParams(
            dimension_semantics=("arbitrary",), vmem_limit_bytes=VMEM
        ),
        name="join",
    )(acc, stat, own)


def project_body(info, got, w_own, w_oth, gate, hidden, cached, out, all_s):
    n = pl.program_id(0)
    prompts, rows, _ = hidden.shape
    part = w_own.shape[0]
    heads = part // 128
    h = info[0]

    @pl.when(n == 0)
    def _():
        for p in range(prompts):
            for k in range(2):
                seat = h if k == 0 else 1 - h
                for j in range(heads):
                    all_s[p * rows : (p + 1) * rows, (k * heads + j) * 128 : (k * heads + j + 1) * 128] = got[
                        (p * SLOTS + j) * 2 + seat
                    ]

    acc = jnp.dot(all_s[:, 0:part], w_own[...], preferred_element_type=F32)
    acc = acc + jnp.dot(all_s[:, part : 2 * part], w_oth[...], preferred_element_type=F32)
    for p in range(prompts):
        y = hidden[p].astype(F32) + gate[p] * acc[p * rows : (p + 1) * rows, :]
        out[p] = (y + cached[p].astype(F32)).astype(BF16)


def project(info, got, w_out, w_oth, gate, hidden, cached):
    prompts, rows, width = hidden.shape
    part = w_out.shape[0]
    bn = 512
    steps = width // bn
    return pl.pallas_call(
        project_body,
        grid_spec=pltpu.PrefetchScalarGridSpec(
            num_scalar_prefetch=1,
            grid=(steps,),
            in_specs=[
                pl.BlockSpec(got.shape, lambda n, s: (0, 0, 0)),
                pl.BlockSpec((part, bn), lambda n, s: (0, s[0] * steps + n)),
                pl.BlockSpec((part, bn), lambda n, s: (0, n)),
                pl.BlockSpec((prompts, 1, bn), lambda n, s: (0, 0, n)),
                pl.BlockSpec((prompts, rows, bn), lambda n, s: (0, 0, n)),
                pl.BlockSpec((prompts, rows, bn), lambda n, s: (0, 0, n)),
            ],
            out_specs=pl.BlockSpec((prompts, rows, bn), lambda n, s: (0, 0, n)),
            scratch_shapes=[pltpu.VMEM((prompts * rows, 2 * part), BF16)],
        ),
        out_shape=jax.ShapeDtypeStruct((prompts, rows, width), BF16),
        compiler_params=pltpu.CompilerParams(
            dimension_semantics=("arbitrary",), vmem_limit_bytes=VMEM
        ),
        cost_estimate=pl.CostEstimate(
            flops=4 * prompts * rows * part * width, bytes_accessed=12_000_000, transcendentals=0
        ),
        name="project",
    )(info, got, w_out, w_oth, gate, hidden, cached)


def per_device(
    image_hidden,
    modulation,
    qkv_weight,
    out_weight,
    q_gain,
    k_gain,
    text_keys,
    text_values,
    stale_keys,
    stale_values,
    cached_residual,
    patch_of,
    refresh,
    text_len,
):
    prompts, rows, width_part = image_hidden.shape
    head_dim = q_gain.shape[0]
    channels = out_weight.shape[0]
    heads = channels // head_dim
    seat = lax.axis_index("seq")
    head_seat = lax.axis_index("head")
    batch_seat = lax.axis_index("batch")
    n_seq = lax.axis_size("seq")
    n_batch = lax.axis_size("batch")
    swap = [(0, 1), (1, 0)]

    other_hidden = lax.ppermute(image_hidden, "head", swap)

    text = jnp.stack([text_keys, text_values], 1)
    t_rows = text.shape[2]
    text = text.reshape(prompts, 2, t_rows, heads, head_dim).transpose(0, 3, 1, 2, 4)
    text = jnp.pad(text, ((0, 0), (0, SLOTS - heads), (0, 0), (0, 0), (0, 0)))
    text = text.reshape(n_seq, 2, t_rows, head_dim)
    text = lax.all_to_all(text, "seq", split_axis=0, concat_axis=0, tiled=True)
    text = text.transpose(1, 0, 2, 3).reshape(2, n_seq * t_rows, head_dim)

    n_y = n_seq // 4
    y_seat = seat // 4
    share = channels // (n_batch * n_y)
    piece = lax.dynamic_slice(
        out_weight,
        ((batch_seat * n_y + y_seat) * share, (1 - head_seat) * width_part),
        (share, width_part),
    )
    piece = lax.ppermute(piece, "head", swap)
    w_y = jnp.zeros((n_y, share, width_part), BF16)
    w_y = lax.dynamic_update_slice(w_y, piece[None], (y_seat, 0, 0))
    for d in range(1, n_y):
        moved = lax.ppermute(piece, "seq", [(i, (i + 4 * d) % n_seq) for i in range(n_seq)])
        w_y = lax.dynamic_update_slice(w_y, moved[None], ((y_seat - d) % n_y, 0, 0))
    w_oth = jnp.zeros((n_batch, n_y, share, width_part), BF16)
    w_oth = lax.dynamic_update_slice(w_oth, w_y[None], (batch_seat, 0, 0, 0))
    for d in range(1, n_batch):
        moved = lax.ppermute(w_y, "batch", [(i, (i + d) % n_batch) for i in range(n_batch)])
        w_oth = lax.dynamic_update_slice(w_oth, moved[None], ((batch_seat - d) % n_batch, 0, 0, 0))
    w_oth = w_oth.reshape(channels, width_part)
    other_hidden, w_oth = lax.optimization_barrier((other_hidden, w_oth))

    seats = jnp.arange(n_seq, dtype=jnp.int32)
    own_band = jnp.sum(jnp.where(seats == seat, patch_of, 0))
    own_flag = jnp.sum(jnp.where(seats == seat, refresh, 0))
    raster = own_band * rows + jnp.arange(rows, dtype=jnp.int32)
    cos, sin = rotary_tables(raster, head_dim, GRID_W)
    info = jnp.stack([head_seat.astype(jnp.int32), own_flag.astype(jnp.int32)])
    send, fresh = qkv(
        info,
        image_hidden,
        other_hidden,
        modulation.transpose(1, 0, 2),
        qkv_weight.transpose(1, 0, 2),
        jnp.stack([q_gain, k_gain]),
        cos,
        sin,
        stale_keys,
        stale_values,
    )
    got = lax.all_to_all(
        send.reshape(n_seq, 3, rows, head_dim), "seq", split_axis=0, concat_axis=0, tiled=True
    )
    own_part = diag(send, fresh)
    unit_prompt = jnp.minimum(seat // SLOTS, prompts - 1)
    length = jnp.sum(jnp.where(jnp.arange(prompts) == unit_prompt, text_len, 0)).astype(jnp.int32)
    acc, stat = attend(length[None], got, text)
    own_part = lax.all_to_all(
        own_part.reshape(n_seq, -1, head_dim), "seq", split_axis=0, concat_axis=0, tiled=True
    )
    back = join(acc, stat, own_part)
    back = lax.all_to_all(
        back.reshape(n_seq * 2, rows, head_dim), ("seq", "head"), split_axis=0, concat_axis=0, tiled=True
    )
    gate = lax.dynamic_slice_in_dim(modulation[:, 2:3], head_seat * width_part, width_part, 2)
    return project(info, back, out_weight, w_oth, gate, image_hidden, cached_residual)


def solution(mesh):
    in_specs = (
        P("batch", "seq", "head"),
        P("batch", None, None),
        P(None, None, "head"),
        P("head", None),
        P(),
        P(),
        P("batch", "seq", "head"),
        P("batch", "seq", "head"),
        P("batch", "seq", "head"),
        P("batch", "seq", "head"),
        P("batch", "seq", "head"),
        P("batch"),
        P("batch"),
        P("batch"),
    )
    out_specs = P("batch", "seq", "head")
    return jax.shard_map(
        per_device, mesh=mesh, in_specs=in_specs, out_specs=out_specs, check_vma=False
    )
```

```python
import jax
import jax.numpy as jnp
from jax import lax
from jax.experimental import pallas as pl
from jax.experimental.pallas import tpu as pltpu
from jax.sharding import PartitionSpec as P


GRID_W = 64
EPS = 1e-06
LOG2E = 1.4426950408889634
F32 = jnp.float32
BF16 = jnp.bfloat16
NEG = -1e30
MIB = 1024 * 1024
SLOTS = 8


def rotary_tables(raster, head_dim, grid_width):
    half_dim = head_dim // 2
    first_pairs = head_dim // 16
    axis_pairs = (half_dim - first_pairs) // 2
    pair_index = jnp.arange(half_dim, dtype=jnp.int32)
    pair_local = jnp.where(
        pair_index < first_pairs + axis_pairs,
        pair_index - first_pairs,
        pair_index - first_pairs - axis_pairs,
    )
    exponent = -pair_local.astype(F32) / float(axis_pairs)
    frequency = jnp.where(pair_index < first_pairs, F32(0.0), jnp.power(F32(10000.0), exponent))
    row_pos = (raster // grid_width).astype(F32)
    col_pos = (raster % grid_width).astype(F32)
    position = jnp.where(
        pair_index[None, :] < first_pairs + axis_pairs, row_pos[:, None], col_pos[:, None]
    )
    angles = position * frequency[None, :]
    cosine = jnp.cos(angles)
    sine = jnp.sin(angles)
    return (jnp.concatenate([cosine, cosine], axis=-1), jnp.concatenate([-sine, sine], axis=-1))


def qkv_body(
    info, own, oth, mod_own, mod_oth, w_own, w_oth, gains, cos, sin, stale_k, stale_v, send, fresh, mod_s
):
    n = pl.program_id(0)
    prompts, rows, part = own.shape
    width = 2 * part
    tile = 16

    @pl.when(n == 0)
    def _():
        for p in range(prompts):
            def norm(i, c):
                at = pl.multiple_of(i * tile, tile)
                a = own[p, pl.ds(at, tile), :].astype(F32)
                b = oth[p, pl.ds(at, tile), :].astype(F32)
                mean = (jnp.sum(a, -1, keepdims=True) + jnp.sum(b, -1, keepdims=True)) / width
                a, b = a - mean, b - mean
                var = (jnp.sum(a * a, -1, keepdims=True) + jnp.sum(b * b, -1, keepdims=True)) / width
                inv = lax.rsqrt(var + EPS)
                a = a * inv * (1.0 + mod_own[1, p : p + 1, :]) + mod_own[0, p : p + 1, :]
                b = b * inv * (1.0 + mod_oth[1, p : p + 1, :]) + mod_oth[0, p : p + 1, :]
                to = pl.multiple_of(p * rows + i * tile, tile)
                mod_s[pl.ds(to, tile), 0:part] = a.astype(BF16)
                mod_s[pl.ds(to, tile), part:width] = b.astype(BF16)
                return c

            lax.fori_loop(0, rows // tile, norm, 0, unroll=4)

    heads = w_own.shape[2] // 128
    per = 2
    flag = info[1]

    def products():
        for j in range(0, heads, per):
            cols = slice(j * 128, (j + per) * 128)
            acc = jnp.dot(mod_s[:, 0:part], w_own[0, :, cols], preferred_element_type=F32)
            acc = acc + jnp.dot(mod_s[:, part:width], w_oth[0, :, cols], preferred_element_type=F32)
            for p in range(prompts):
                for e in range(per):
                    yield p, j + e, acc[p * rows : (p + 1) * rows, e * 128 : (e + 1) * 128]

    def turned(x, gain):
        x = x * lax.rsqrt(jnp.mean(x * x, axis=-1, keepdims=True) + EPS) * gain
        return x * cos[...] + pltpu.roll(x, 64, 1) * sin[...]

    @pl.when(n == 0)
    def _():
        for p, j, x in products():
            send[p, j, 0] = turned(x, gains[0:1, :]).astype(BF16)

    @pl.when(n == 1)
    def _():
        for p, j, x in products():
            new = turned(x, gains[1:2, :]).astype(BF16)
            fresh[p, j, 0] = new
            send[p, j, 0] = jnp.where(flag == 1, new, stale_k[p, :, j * 128 : (j + 1) * 128])

    @pl.when(n == 2)
    def _():
        for p, j, x in products():
            new = x.astype(BF16)
            used = jnp.where(flag == 1, new, stale_v[p, :, j * 128 : (j + 1) * 128])
            for r in range(0, rows, 128):
                fresh[p, j, 0, r : r + 128, :] = jnp.transpose(new[r : r + 128, :])
                send[p, j, 0, r : r + 128, :] = jnp.transpose(used[r : r + 128, :])


def qkv(info, own, oth, modulation, w, gains, cos, sin, stale_k, stale_v):
    prompts, rows, part = own.shape
    channels = stale_k.shape[2]
    heads = channels // 128
    whole = lambda *shape: pl.BlockSpec(shape, lambda n, s: (0,) * len(shape))
    return pl.pallas_call(
        qkv_body,
        grid_spec=pltpu.PrefetchScalarGridSpec(
            num_scalar_prefetch=1,
            grid=(3,),
            in_specs=[
                whole(prompts, rows, part),
                whole(prompts, rows, part),
                pl.BlockSpec((3, prompts, part), lambda n, s: (0, 0, s[0])),
                pl.BlockSpec((3, prompts, part), lambda n, s: (0, 0, 1 - s[0])),
                pl.BlockSpec((1, part, channels), lambda n, s: (n, s[0], 0)),
                pl.BlockSpec((1, part, channels), lambda n, s: (n, 1 - s[0], 0)),
                whole(2, 128),
                whole(rows, 128),
                whole(rows, 128),
                whole(prompts, rows, channels),
                whole(prompts, rows, channels),
            ],
            out_specs=[
                pl.BlockSpec((prompts, SLOTS, 1, rows, 128), lambda n, s: (0, 0, n, 0, 0)),
                pl.BlockSpec(
                    (prompts, heads, 1, rows, 128), lambda n, s: (0, 0, jnp.maximum(n - 1, 0), 0, 0)
                ),
            ],
            scratch_shapes=[pltpu.VMEM((prompts * rows, 2 * part), BF16)],
        ),
        out_shape=[
            jax.ShapeDtypeStruct((prompts, SLOTS, 3, rows, 128), BF16),
            jax.ShapeDtypeStruct((prompts, heads, 2, rows, 128), BF16),
        ],
        compiler_params=pltpu.CompilerParams(
            dimension_semantics=("arbitrary",), vmem_limit_bytes=36 * MIB
        ),
        cost_estimate=pl.CostEstimate(
            flops=2 * prompts * rows * 2 * part * 3 * channels, bytes_accessed=20_000_000, transcendentals=0
        ),
        name="qkv",
    )(info, own, oth, modulation, modulation, w, w, gains, cos, sin, stale_k, stale_v)


def side_by_side(ref, at):
    rows = ref.shape[-2]
    return jnp.concatenate([ref[(*at, slice(r, r + 128), slice(None))] for r in range(0, rows, 128)], 1)


CONTRACT = (((1,), (1,)), ((), ()))


def diag_body(q, kv, out):
    c = 128**-0.5 * LOG2E
    rows = q.shape[3]
    for e in range(q.shape[1]):
        s = lax.dot_general(kv[0, e, 0], q[0, e, 0], CONTRACT, preferred_element_type=F32) * c
        top = jnp.max(s, axis=0, keepdims=True)
        w = jnp.exp2(s - top)
        total = jnp.sum(w, axis=0, keepdims=True)
        o = jnp.dot(side_by_side(kv, (0, e, 1)), w.astype(BF16), preferred_element_type=F32)
        out[0, e, 0:128, :] = (o / total).astype(BF16)
        lse = jnp.broadcast_to(top + jnp.log2(total), (16, rows))
        first = lse.astype(BF16).astype(F32)
        second = (lse - first).astype(BF16).astype(F32)
        third = lse - first - second
        at = lax.broadcasted_iota(jnp.int32, lse.shape, 0)
        out[0, e, 128:144, :] = jnp.where(at == 0, first, jnp.where(at == 1, second, third)).astype(BF16)


def diag(send, fresh):
    prompts, heads, _, rows, _ = fresh.shape
    return pl.pallas_call(
        diag_body,
        grid=(prompts,),
        in_specs=[
            pl.BlockSpec((1, heads, 1, rows, 128), lambda p: (p, 0, 0, 0, 0)),
            pl.BlockSpec((1, heads, 2, rows, 128), lambda p: (p, 0, 0, 0, 0)),
        ],
        out_specs=pl.BlockSpec((1, SLOTS, 144, rows), lambda p: (p, 0, 0, 0)),
        out_shape=jax.ShapeDtypeStruct((prompts, SLOTS, 144, rows), BF16),
        compiler_params=pltpu.CompilerParams(
            dimension_semantics=("arbitrary",), vmem_limit_bytes=16 * MIB
        ),
        cost_estimate=pl.CostEstimate(
            flops=4 * prompts * heads * rows * rows * 128,
            bytes_accessed=4_000_000,
            transcendentals=prompts * heads * rows * rows,
        ),
        name="diag",
    )(send, fresh)


def attend_body(info, got, text_k, text_v, out, stat, s_even, s_odd, top_s):
    g = pl.program_id(0)
    blocks, _, rows, _ = got.shape
    c = 128**-0.5 * LOG2E
    lead = text_k.shape[0] // rows
    tiles = lead + blocks - 1
    groups = [list(range(i, min(i + 4, tiles))) for i in range(0, tiles, 4)]
    if len(groups[-1]) == 1:
        last = groups.pop()
        groups[-1] = groups[-1] + last

    def block_of(b, i):
        return lax.rem(b + 1 + (i - lead), blocks)

    def keys(b, i):
        return text_k[i * rows : (i + 1) * rows, :] if i < lead else got[block_of(b, i), 1]

    def values(b, i):
        return text_v[:, i * rows : (i + 1) * rows] if i < lead else side_by_side(got, (block_of(b, i), 2))

    def score(b, group, top, s_ref):
        k = jnp.concatenate([keys(b, i) for i in group], 0)
        scores = lax.dot_general(k, got[b, 0], CONTRACT, preferred_element_type=F32)
        for m, i in enumerate(group):
            s = scores[m * rows : (m + 1) * rows, :]
            if i < lead:
                at = i * rows + lax.broadcasted_iota(jnp.int32, s.shape, 0)
                s = jnp.where(at < info[0], s, NEG)
            s_ref[i] = s
            part = jnp.max(s.reshape(rows // 8, 8, rows), axis=0)
            top = part if top is None else jnp.maximum(top, part)
        return top

    def whole_top(top):
        return jnp.broadcast_to(jnp.max(top, axis=0, keepdims=True) * c, (8, rows))

    @pl.when(g == 0)
    def _():
        top = None
        for group in groups:
            top = score(0, group, top, s_even)
        top_s[...] = whole_top(top)

    top = top_s[...]
    for k in range(2):
        b = 2 * g + k
        nxt = lax.rem(b + 1, blocks)
        here, there = (s_even, s_odd) if k == 0 else (s_odd, s_even)
        total = None
        acc = None
        nxt_top = None
        for group in groups:
            nxt_top = score(nxt, group, nxt_top, there)
            w = []
            for i in group:
                x = jnp.exp2(here[i] * c - top[0:1, :])
                part = jnp.sum(x.reshape(rows // 8, 8, rows), axis=0)
                total = part if total is None else total + part
                w.append(x.astype(BF16))
            v = jnp.concatenate([values(b, i) for i in group], 1)
            o = jnp.dot(v, jnp.concatenate(w, 0), preferred_element_type=F32)
            acc = o if acc is None else acc + o
        out[k] = acc
        total = jnp.broadcast_to(jnp.sum(total, axis=0, keepdims=True), (8, rows))
        at = lax.broadcasted_iota(jnp.int32, (8, rows), 0)
        stat[k] = jnp.where(at < 4, top, total)
        top = whole_top(nxt_top)
    top_s[...] = top


def attend(info, got, text_k, text_v):
    blocks, _, rows, _ = got.shape
    tiles = text_k.shape[0] // rows + blocks - 1
    return pl.pallas_call(
        attend_body,
        grid_spec=pltpu.PrefetchScalarGridSpec(
            num_scalar_prefetch=1,
            grid=(blocks // 2,),
            in_specs=[
                pl.BlockSpec(got.shape, lambda b, s: (0, 0, 0, 0)),
                pl.BlockSpec(text_k.shape, lambda b, s: (0, 0)),
                pl.BlockSpec(text_v.shape, lambda b, s: (0, 0)),
            ],
            out_specs=[
                pl.BlockSpec((2, 128, rows), lambda b, s: (b, 0, 0)),
                pl.BlockSpec((2, 8, rows), lambda b, s: (b, 0, 0)),
            ],
            scratch_shapes=[
                pltpu.VMEM((tiles, rows, rows), F32),
                pltpu.VMEM((tiles, rows, rows), F32),
                pltpu.VMEM((8, rows), F32),
            ],
        ),
        out_shape=[
            jax.ShapeDtypeStruct((blocks, 128, rows), F32),
            jax.ShapeDtypeStruct((blocks, 8, rows), F32),
        ],
        compiler_params=pltpu.CompilerParams(
            dimension_semantics=("arbitrary",), vmem_limit_bytes=32 * MIB
        ),
        cost_estimate=pl.CostEstimate(
            flops=4 * blocks * rows * tiles * rows * 128 * 2,
            bytes_accessed=8_000_000,
            transcendentals=blocks * rows * tiles * rows,
        ),
        name="attend",
    )(info, got, text_k, text_v)


def join_body(acc, stat, own, out):
    for e in range(acc.shape[0]):
        top = stat[e, 0:1, :]
        total = stat[e, 4:5, :]
        pieces = own[e, 128:144, :].astype(F32)
        other = pieces[0:1, :] + pieces[1:2, :] + pieces[2:3, :]
        high = jnp.maximum(other, top)
        u = jnp.exp2(top - high)
        w = jnp.exp2(other - high)
        o = (acc[e] * u + own[e, 0:128, :].astype(F32) * w) / (total * u + w)
        o = jnp.transpose(o).astype(BF16)
        out[e, 0] = o
        out[e, 1] = o


def join(acc, stat, own):
    blocks, _, rows = acc.shape
    per = 4
    return pl.pallas_call(
        join_body,
        grid=(blocks // per,),
        in_specs=[
            pl.BlockSpec((per, 128, rows), lambda b: (b, 0, 0)),
            pl.BlockSpec((per, 8, rows), lambda b: (b, 0, 0)),
            pl.BlockSpec((per, 144, rows), lambda b: (b, 0, 0)),
        ],
        out_specs=pl.BlockSpec((per, 2, rows, 128), lambda b: (b, 0, 0, 0)),
        out_shape=jax.ShapeDtypeStruct((blocks, 2, rows, 128), BF16),
        compiler_params=pltpu.CompilerParams(
            dimension_semantics=("arbitrary",), vmem_limit_bytes=16 * MIB
        ),
        name="join",
    )(acc, stat, own)


def project_body(info, got, w_own, w_oth, gate, hidden, cached, out, all_s):
    n = pl.program_id(0)
    prompts, rows, _ = hidden.shape
    part = w_own.shape[0]
    heads = part // 128
    h = info[0]

    @pl.when(n == 0)
    def _():
        for p in range(prompts):
            for k in range(2):
                seat = h if k == 0 else 1 - h
                for j in range(heads):
                    all_s[p * rows : (p + 1) * rows, (k * heads + j) * 128 : (k * heads + j + 1) * 128] = got[
                        (p * SLOTS + j) * 2 + seat
                    ]

    acc = jnp.dot(all_s[:, 0:part], w_own[...], preferred_element_type=F32)
    acc = acc + jnp.dot(all_s[:, part : 2 * part], w_oth[...], preferred_element_type=F32)
    for p in range(prompts):
        y = hidden[p].astype(F32) + gate[p] * acc[p * rows : (p + 1) * rows, :]
        out[p] = (y + cached[p].astype(F32)).astype(BF16)


def project(info, got, w_out, w_oth, gate, hidden, cached):
    prompts, rows, width = hidden.shape
    part = w_out.shape[0]
    bn = 512
    steps = width // bn
    return pl.pallas_call(
        project_body,
        grid_spec=pltpu.PrefetchScalarGridSpec(
            num_scalar_prefetch=1,
            grid=(steps,),
            in_specs=[
                pl.BlockSpec(got.shape, lambda n, s: (0, 0, 0)),
                pl.BlockSpec((part, bn), lambda n, s: (0, s[0] * steps + n)),
                pl.BlockSpec((part, bn), lambda n, s: (0, n)),
                pl.BlockSpec((prompts, 1, bn), lambda n, s: (0, 0, n)),
                pl.BlockSpec((prompts, rows, bn), lambda n, s: (0, 0, n)),
                pl.BlockSpec((prompts, rows, bn), lambda n, s: (0, 0, n)),
            ],
            out_specs=pl.BlockSpec((prompts, rows, bn), lambda n, s: (0, 0, n)),
            scratch_shapes=[pltpu.VMEM((prompts * rows, 2 * part), BF16)],
        ),
        out_shape=jax.ShapeDtypeStruct((prompts, rows, width), BF16),
        compiler_params=pltpu.CompilerParams(
            dimension_semantics=("arbitrary",), vmem_limit_bytes=20 * MIB
        ),
        cost_estimate=pl.CostEstimate(
            flops=4 * prompts * rows * part * width, bytes_accessed=12_000_000, transcendentals=0
        ),
        name="project",
    )(info, got, w_out, w_oth, gate, hidden, cached)


def per_device(
    image_hidden,
    modulation,
    qkv_weight,
    out_weight,
    q_gain,
    k_gain,
    text_keys,
    text_values,
    stale_keys,
    stale_values,
    cached_residual,
    patch_of,
    refresh,
    text_len,
):
    prompts, rows, width_part = image_hidden.shape
    head_dim = q_gain.shape[0]
    channels = out_weight.shape[0]
    heads = channels // head_dim
    seat = lax.axis_index("seq")
    head_seat = lax.axis_index("head")
    batch_seat = lax.axis_index("batch")
    n_seq = lax.axis_size("seq")
    n_batch = lax.axis_size("batch")
    swap = [(0, 1), (1, 0)]

    other_hidden = lax.ppermute(image_hidden, "head", swap)

    text = jnp.stack([text_keys, text_values], 1)
    t_rows = text.shape[2]
    text = text.reshape(prompts, 2, t_rows, heads, head_dim).transpose(0, 3, 1, 2, 4)
    text = jnp.pad(text, ((0, 0), (0, SLOTS - heads), (0, 0), (0, 0), (0, 0)))
    text = text.reshape(n_seq, 2, t_rows, head_dim)
    text = lax.all_to_all(text, "seq", split_axis=0, concat_axis=0, tiled=True)
    text_k = text[:, 0].reshape(n_seq * t_rows, head_dim)
    text_v = text[:, 1].reshape(n_seq * t_rows, head_dim).T

    n_y = n_seq // 4
    y_seat = seat // 4
    share = channels // (n_batch * n_y)
    piece = lax.dynamic_slice(
        out_weight,
        ((batch_seat * n_y + y_seat) * share, (1 - head_seat) * width_part),
        (share, width_part),
    )
    piece = lax.ppermute(piece, "head", swap)
    w_y = jnp.zeros((n_y, share, width_part), BF16)
    w_y = lax.dynamic_update_slice(w_y, piece[None], (y_seat, 0, 0))
    for d in range(1, n_y):
        moved = lax.ppermute(piece, "seq", [(i, (i + 4 * d) % n_seq) for i in range(n_seq)])
        w_y = lax.dynamic_update_slice(w_y, moved[None], ((y_seat - d) % n_y, 0, 0))
    other_hidden, w_y = lax.optimization_barrier((other_hidden, w_y))
    w_oth = jnp.zeros((n_batch, n_y, share, width_part), BF16)
    w_oth = lax.dynamic_update_slice(w_oth, w_y[None], (batch_seat, 0, 0, 0))
    for d in range(1, n_batch):
        moved = lax.ppermute(w_y, "batch", [(i, (i + d) % n_batch) for i in range(n_batch)])
        w_oth = lax.dynamic_update_slice(w_oth, moved[None], ((batch_seat - d) % n_batch, 0, 0, 0))
    w_oth = w_oth.reshape(channels, width_part)
    text_k, w_oth = lax.optimization_barrier((text_k, w_oth))

    seats = jnp.arange(n_seq, dtype=jnp.int32)
    own_band = jnp.sum(jnp.where(seats == seat, patch_of, 0))
    own_flag = jnp.sum(jnp.where(seats == seat, refresh, 0))
    raster = own_band * rows + jnp.arange(rows, dtype=jnp.int32)
    cos, sin = rotary_tables(raster, head_dim, GRID_W)
    info = jnp.stack([head_seat.astype(jnp.int32), own_flag.astype(jnp.int32)])
    send, fresh = qkv(
        info,
        image_hidden,
        other_hidden,
        modulation.transpose(1, 0, 2),
        qkv_weight.transpose(1, 0, 2),
        jnp.stack([q_gain, k_gain]),
        cos,
        sin,
        stale_keys,
        stale_values,
    )
    got = lax.all_to_all(
        send.reshape(n_seq, 3, rows, head_dim), "seq", split_axis=0, concat_axis=0, tiled=True
    )
    own_part = diag(send, fresh)
    unit_prompt = jnp.minimum(seat // SLOTS, prompts - 1)
    length = jnp.sum(jnp.where(jnp.arange(prompts) == unit_prompt, text_len, 0)).astype(jnp.int32)
    acc, stat = attend(length[None], got, text_k, text_v)
    own_part = lax.all_to_all(
        own_part.reshape(n_seq, -1, rows), "seq", split_axis=0, concat_axis=0, tiled=True
    )
    back = join(acc, stat, own_part)
    back = lax.all_to_all(
        back.reshape(n_seq * 2, rows, head_dim), ("seq", "head"), split_axis=0, concat_axis=0, tiled=True
    )
    gate = lax.dynamic_slice_in_dim(modulation[:, 2:3], head_seat * width_part, width_part, 2)
    return project(info, back, out_weight, w_oth, gate, image_hidden, cached_residual)


def solution(mesh):
    in_specs = (
        P("batch", "seq", "head"),
        P("batch", None, None),
        P(None, None, "head"),
        P("head", None),
        P(),
        P(),
        P("batch", "seq", "head"),
        P("batch", "seq", "head"),
        P("batch", "seq", "head"),
        P("batch", "seq", "head"),
        P("batch", "seq", "head"),
        P("batch"),
        P("batch"),
        P("batch"),
    )
    out_specs = P("batch", "seq", "head")
    return jax.shard_map(
        per_device, mesh=mesh, in_specs=in_specs, out_specs=out_specs, check_vma=False
    )
```

```python
import jax
import jax.numpy as jnp
from jax import lax
from jax.experimental import pallas as pl
from jax.experimental.pallas import tpu as pltpu
from jax.sharding import PartitionSpec as P


GRID_W = 64
EPS = 1e-06
LOG2E = 1.4426950408889634
F32 = jnp.float32
BF16 = jnp.bfloat16
NEG = -1e30
VMEM = 56 * 1024 * 1024
SLOTS = 8


def rotary_tables(raster, head_dim, grid_width):
    half_dim = head_dim // 2
    first_pairs = head_dim // 16
    axis_pairs = (half_dim - first_pairs) // 2
    pair_index = jnp.arange(half_dim, dtype=jnp.int32)
    pair_local = jnp.where(
        pair_index < first_pairs + axis_pairs,
        pair_index - first_pairs,
        pair_index - first_pairs - axis_pairs,
    )
    exponent = -pair_local.astype(F32) / float(axis_pairs)
    frequency = jnp.where(pair_index < first_pairs, F32(0.0), jnp.power(F32(10000.0), exponent))
    row_pos = (raster // grid_width).astype(F32)
    col_pos = (raster % grid_width).astype(F32)
    position = jnp.where(
        pair_index[None, :] < first_pairs + axis_pairs, row_pos[:, None], col_pos[:, None]
    )
    angles = position * frequency[None, :]
    cosine = jnp.cos(angles)
    sine = jnp.sin(angles)
    return (jnp.concatenate([cosine, cosine], axis=-1), jnp.concatenate([-sine, sine], axis=-1))


def qkv_body(
    info, own, oth, mod_own, mod_oth, w_own, w_oth, gains, cos, sin, stale_k, stale_v, send, fresh, mod_s, wide_s
):
    n = pl.program_id(0)
    prompts, rows, part = own.shape
    width = 2 * part
    tile = 16

    @pl.when(n == 0)
    def _():
        for p in range(prompts):
            for k in range(2):
                for m, mod in enumerate((mod_own, mod_oth)):
                    row = mod[k, p : p + 1, :] + float(k)
                    wide_s[k, :, m * part : (m + 1) * part] = jnp.broadcast_to(row, (8, part))

            def norm(i, c):
                at = pl.multiple_of(i * tile, tile)
                a = own[p, pl.ds(at, tile), :].astype(F32)
                b = oth[p, pl.ds(at, tile), :].astype(F32)
                mean = (jnp.sum(a, -1, keepdims=True) + jnp.sum(b, -1, keepdims=True)) / width
                a, b = a - mean, b - mean
                var = (jnp.sum(a * a, -1, keepdims=True) + jnp.sum(b * b, -1, keepdims=True)) / width
                inv = lax.rsqrt(var + EPS)
                a = moved(a * inv, 0)
                b = moved(b * inv, part)
                to = pl.multiple_of(p * rows + i * tile, tile)
                mod_s[pl.ds(to, tile), 0:part] = a.astype(BF16)
                mod_s[pl.ds(to, tile), part:width] = b.astype(BF16)
                return c

            def moved(x, at):
                shift, scale = (wide_s[k, :, at : at + part] for k in range(2))
                parts = [x[r : r + 8] * scale + shift for r in range(0, tile, 8)]
                return jnp.concatenate(parts, 0)

            lax.fori_loop(0, rows // tile, norm, 0, unroll=4)

    heads = w_own.shape[2] // 128
    per = 2
    flag = info[1]

    def products():
        for j in range(0, heads, per):
            cols = slice(j * 128, (j + per) * 128)
            acc = jnp.dot(mod_s[:, 0:part], w_own[0, :, cols], preferred_element_type=F32)
            acc = acc + jnp.dot(mod_s[:, part:width], w_oth[0, :, cols], preferred_element_type=F32)
            for p in range(prompts):
                for e in range(per):
                    yield p, j + e, acc[p * rows : (p + 1) * rows, e * 128 : (e + 1) * 128]

    def turned(x, gain):
        x = x * lax.rsqrt(jnp.mean(x * x, axis=-1, keepdims=True) + EPS) * gain
        return x * cos[...] + pltpu.roll(x, 64, 1) * sin[...]

    @pl.when(n == 0)
    def _():
        for p, j, x in products():
            send[p, j, 0] = turned(x, gains[0:1, :]).astype(BF16)

    @pl.when(n == 1)
    def _():
        for p, j, x in products():
            new = turned(x, gains[1:2, :]).astype(BF16)
            fresh[p, j, 0] = new
            send[p, j, 0] = jnp.where(flag == 1, new, stale_k[p, :, j * 128 : (j + 1) * 128])

    @pl.when(n == 2)
    def _():
        for p, j, x in products():
            new = x.astype(BF16)
            used = jnp.where(flag == 1, new, stale_v[p, :, j * 128 : (j + 1) * 128])
            for r in range(0, rows, 128):
                fresh[p, j, 0, r : r + 128, :] = jnp.transpose(new[r : r + 128, :])
                send[p, j, 0, r : r + 128, :] = jnp.transpose(used[r : r + 128, :])


def qkv(c, info, own, oth, modulation, w, gains, cos, sin, stale_k, stale_v):
    prompts, rows, part = oth.shape
    channels = stale_k.shape[2]
    heads = channels // 128
    whole = lambda *shape: pl.BlockSpec(shape, lambda n, s: (0,) * len(shape))
    half = lambda *shape: pl.BlockSpec(shape, lambda n, s: (0, c, 0))
    return pl.pallas_call(
        qkv_body,
        grid_spec=pltpu.PrefetchScalarGridSpec(
            num_scalar_prefetch=1,
            grid=(3,),
            in_specs=[
                half(prompts, rows, part),
                whole(prompts, rows, part),
                pl.BlockSpec((3, prompts, part), lambda n, s: (0, 0, s[0])),
                pl.BlockSpec((3, prompts, part), lambda n, s: (0, 0, 1 - s[0])),
                pl.BlockSpec((1, part, channels), lambda n, s: (n, s[0], 0)),
                pl.BlockSpec((1, part, channels), lambda n, s: (n, 1 - s[0], 0)),
                whole(2, 128),
                pl.BlockSpec((rows, 128), lambda n, s: (c, 0)),
                pl.BlockSpec((rows, 128), lambda n, s: (c, 0)),
                half(prompts, rows, channels),
                half(prompts, rows, channels),
            ],
            out_specs=[
                pl.BlockSpec((prompts, SLOTS, 1, rows, 128), lambda n, s: (0, 0, n, 0, 0)),
                pl.BlockSpec(
                    (prompts, heads, 1, rows, 128), lambda n, s: (0, 0, jnp.maximum(n - 1, 0), 0, 0)
                ),
            ],
            scratch_shapes=[
                pltpu.VMEM((prompts * rows, 2 * part), BF16),
                pltpu.VMEM((2, 8, 2 * part), F32),
            ],
        ),
        out_shape=[
            jax.ShapeDtypeStruct((prompts, SLOTS, 3, rows, 128), BF16),
            jax.ShapeDtypeStruct((prompts, heads, 2, rows, 128), BF16),
        ],
        compiler_params=pltpu.CompilerParams(
            dimension_semantics=("arbitrary",), vmem_limit_bytes=VMEM
        ),
        cost_estimate=pl.CostEstimate(
            flops=2 * prompts * rows * 2 * part * 3 * channels, bytes_accessed=20_000_000, transcendentals=0
        ),
        name="qkv",
    )(info, own, oth, modulation, modulation, w, w, gains, cos, sin, stale_k, stale_v)


CONTRACT = (((1,), (1,)), ((), ()))


def log_sum_rows(lse):
    lse = jnp.broadcast_to(lse, (16, lse.shape[1]))
    first = lse.astype(BF16).astype(F32)
    second = (lse - first).astype(BF16).astype(F32)
    third = lse - first - second
    at = lax.broadcasted_iota(jnp.int32, lse.shape, 0)
    return jnp.where(at == 0, first, jnp.where(at == 1, second, third)).astype(BF16)


def diag_body(*refs):
    halves = len(refs) // 2
    send, fresh, out = refs[:halves], refs[halves : 2 * halves], refs[-1]
    c = 128**-0.5 * LOG2E
    for e in range(out.shape[1]):
        q = jnp.concatenate([r[0, e, 0] for r in send], 0)
        k = jnp.concatenate([r[0, e, 0] for r in fresh], 0)
        v = jnp.concatenate([r[0, e, 1] for r in fresh], 1)
        s = lax.dot_general(k, q, CONTRACT, preferred_element_type=F32) * c
        top = jnp.max(s, axis=0, keepdims=True)
        w = jnp.exp2(s - top)
        total = jnp.sum(w, axis=0, keepdims=True)
        o = jnp.dot(v, w.astype(BF16), preferred_element_type=F32)
        out[0, e, 0:128, :] = (o / total).astype(BF16)
        out[0, e, 128:144, :] = log_sum_rows(top + jnp.log2(total))


def diag(send, fresh):
    prompts, heads, _, part, _ = fresh[0].shape
    rows = part * len(send)
    return pl.pallas_call(
        diag_body,
        grid=(prompts,),
        in_specs=[pl.BlockSpec((1, heads, 1, part, 128), lambda p: (p, 0, 0, 0, 0))] * len(send)
        + [pl.BlockSpec((1, heads, 2, part, 128), lambda p: (p, 0, 0, 0, 0))] * len(send),
        out_specs=pl.BlockSpec((1, heads, 144, rows), lambda p: (p, 0, 0, 0)),
        out_shape=jax.ShapeDtypeStruct((prompts, heads, 144, rows), BF16),
        compiler_params=pltpu.CompilerParams(
            dimension_semantics=("arbitrary",), vmem_limit_bytes=VMEM
        ),
        cost_estimate=pl.CostEstimate(
            flops=4 * prompts * heads * rows * rows * 128,
            bytes_accessed=4_000_000,
            transcendentals=prompts * heads * rows * rows,
        ),
        name="diag",
    )(*send, *fresh)


def attend_body(info, got_0, got_1, text_k, text_v, out, s_even, s_odd, top_s):
    g = pl.program_id(0)
    got = (got_0, got_1)
    blocks = got_0.shape[0]
    rows = 2 * got_0.shape[2]
    c = 128**-0.5 * LOG2E
    lead = text_k.shape[0] // rows
    tiles = lead + blocks - 1
    groups = [list(range(i, min(i + 4, tiles))) for i in range(0, tiles, 4)]
    if len(groups[-1]) == 1:
        last = groups.pop()
        groups[-1] = groups[-1] + last

    def block_of(b, i):
        return lax.rem(b + 1 + (i - lead), blocks)

    def keys(b, i):
        if i < lead:
            return [text_k[i * rows : (i + 1) * rows, :]]
        return [r[block_of(b, i), 1] for r in got]

    def values(b, i):
        if i < lead:
            return [text_v[:, i * rows : (i + 1) * rows]]
        return [r[block_of(b, i), 2] for r in got]

    def score(b, group, top, s_ref):
        k = jnp.concatenate([x for i in group for x in keys(b, i)], 0)
        q = jnp.concatenate([r[b, 0] for r in got], 0)
        scores = lax.dot_general(k, q, CONTRACT, preferred_element_type=F32)
        for m, i in enumerate(group):
            s = scores[m * rows : (m + 1) * rows, :]
            if i < lead:
                at = i * rows + lax.broadcasted_iota(jnp.int32, s.shape, 0)
                s = jnp.where(at < info[0], s, NEG)
            s_ref[i] = s
            part = jnp.max(s.reshape(rows // 8, 8, rows), axis=0)
            top = part if top is None else jnp.maximum(top, part)
        return top

    def whole_top(top):
        return jnp.broadcast_to(jnp.max(top, axis=0, keepdims=True) * c, (8, rows))

    @pl.when(g == 0)
    def _():
        top = None
        for group in groups:
            top = score(0, group, top, s_even)
        top_s[...] = whole_top(top)

    top = top_s[...]
    for k in range(2):
        b = 2 * g + k
        nxt = lax.rem(b + 1, blocks)
        here, there = (s_even, s_odd) if k == 0 else (s_odd, s_even)
        total = None
        acc = None
        nxt_top = None
        late = None

        def product(acc, late):
            group, w = late
            v = jnp.concatenate([x for i in group for x in values(b, i)], 1)
            o = jnp.dot(v, w, preferred_element_type=F32)
            return o if acc is None else acc + o

        for group in groups:
            nxt_top = score(nxt, group, nxt_top, there)
            w = []
            for i in group:
                x = jnp.exp2(here[i] * c - top[0:1, :])
                part = jnp.sum(x.reshape(rows // 8, 8, rows), axis=0)
                total = part if total is None else total + part
                w.append(x.astype(BF16))
            if late is not None:
                acc = product(acc, late)
            late = (group, jnp.concatenate(w, 0))
        acc = product(acc, late)
        total = jnp.sum(total, axis=0, keepdims=True)
        acc = (acc / total).astype(BF16)
        lse = log_sum_rows(top[0:1, :] + jnp.log2(total))
        for seat in range(2):
            out[k, seat, 0:128, :] = acc
            out[k, seat, 128:144, :] = lse
        top = whole_top(nxt_top)
    top_s[...] = top


def attend(info, got, text_k, text_v):
    blocks, _, part, _ = got[0].shape
    rows = part * len(got)
    tiles = text_k.shape[0] // rows + blocks - 1
    return pl.pallas_call(
        attend_body,
        grid_spec=pltpu.PrefetchScalarGridSpec(
            num_scalar_prefetch=1,
            grid=(blocks // 2,),
            in_specs=[
                pl.BlockSpec(got[0].shape, lambda b, s: (0, 0, 0, 0)),
                pl.BlockSpec(got[1].shape, lambda b, s: (0, 0, 0, 0)),
                pl.BlockSpec(text_k.shape, lambda b, s: (0, 0)),
                pl.BlockSpec(text_v.shape, lambda b, s: (0, 0)),
            ],
            out_specs=pl.BlockSpec((2, 2, 144, rows), lambda b, s: (b, 0, 0, 0)),
            scratch_shapes=[
                pltpu.VMEM((tiles, rows, rows), F32),
                pltpu.VMEM((tiles, rows, rows), F32),
                pltpu.VMEM((8, rows), F32),
            ],
        ),
        out_shape=jax.ShapeDtypeStruct((blocks, 2, 144, rows), BF16),
        compiler_params=pltpu.CompilerParams(
            dimension_semantics=("arbitrary",), vmem_limit_bytes=VMEM
        ),
        cost_estimate=pl.CostEstimate(
            flops=4 * blocks * rows * tiles * rows * 128 * 2,
            bytes_accessed=8_000_000,
            transcendentals=blocks * rows * tiles * rows,
        ),
        name="attend",
    )(info, *got, text_k, text_v)


def project_body(info, got, near, far, w_own, w_oth, gate, hidden, cached, out, all_s):
    n = pl.program_id(0)
    prompts, rows, _ = hidden.shape
    part = w_own.shape[0]
    heads = part // 128
    h = info[0]

    def log_sum(x):
        x = x.astype(F32)
        return x[0:1, :] + x[1:2, :] + x[2:3, :]

    @pl.when(n == 0)
    def _():
        for p in range(prompts):
            for k in range(2):
                own = (near, far)[k]
                seat = h if k == 0 else 1 - h
                for j in range(heads):
                    at = (p * SLOTS + j) * 2 + seat
                    a = log_sum(got[at, 128:144, :])
                    b = log_sum(own[p, j, 128:144, :])
                    high = jnp.maximum(a, b)
                    a, b = jnp.exp2(a - high), jnp.exp2(b - high)
                    o = (got[at, 0:128, :].astype(F32) * a + own[p, j, 0:128, :].astype(F32) * b) / (a + b)
                    col = (k * heads + j) * 128
                    all_s[p * rows : (p + 1) * rows, col : col + 128] = jnp.transpose(o.astype(BF16))

    acc = jnp.dot(all_s[:, 0:part], w_own[...], preferred_element_type=F32)
    acc = acc + jnp.dot(all_s[:, part : 2 * part], w_oth[...], preferred_element_type=F32)
    for p in range(prompts):
        y = hidden[p].astype(F32) + gate[p] * acc[p * rows : (p + 1) * rows, :]
        out[p] = (y + cached[p].astype(F32)).astype(BF16)


def project(info, got, near, far, w_out, w_oth, gate, hidden, cached):
    prompts, rows, width = hidden.shape
    part = w_out.shape[0]
    bn = 512
    steps = width // bn
    return pl.pallas_call(
        project_body,
        grid_spec=pltpu.PrefetchScalarGridSpec(
            num_scalar_prefetch=1,
            grid=(steps,),
            in_specs=[
                pl.BlockSpec(got.shape, lambda n, s: (0, 0, 0)),
                pl.BlockSpec(near.shape, lambda n, s: (0, 0, 0, 0)),
                pl.BlockSpec(far.shape, lambda n, s: (0, 0, 0, 0)),
                pl.BlockSpec((part, bn), lambda n, s: (0, s[0] * steps + n)),
                pl.BlockSpec((part, bn), lambda n, s: (0, n)),
                pl.BlockSpec((prompts, 1, bn), lambda n, s: (0, 0, n)),
                pl.BlockSpec((prompts, rows, bn), lambda n, s: (0, 0, n)),
                pl.BlockSpec((prompts, rows, bn), lambda n, s: (0, 0, n)),
            ],
            out_specs=pl.BlockSpec((prompts, rows, bn), lambda n, s: (0, 0, n)),
            scratch_shapes=[pltpu.VMEM((prompts * rows, 2 * part), BF16)],
        ),
        out_shape=jax.ShapeDtypeStruct((prompts, rows, width), BF16),
        compiler_params=pltpu.CompilerParams(
            dimension_semantics=("arbitrary",), vmem_limit_bytes=VMEM
        ),
        cost_estimate=pl.CostEstimate(
            flops=4 * prompts * rows * part * width, bytes_accessed=12_000_000, transcendentals=0
        ),
        name="project",
    )(info, got, near, far, w_out, w_oth, gate, hidden, cached)


def per_device(
    image_hidden,
    modulation,
    qkv_weight,
    out_weight,
    q_gain,
    k_gain,
    text_keys,
    text_values,
    stale_keys,
    stale_values,
    cached_residual,
    patch_of,
    refresh,
    text_len,
):
    prompts, rows, width_part = image_hidden.shape
    head_dim = q_gain.shape[0]
    channels = out_weight.shape[0]
    heads = channels // head_dim
    seat = lax.axis_index("seq")
    head_seat = lax.axis_index("head")
    batch_seat = lax.axis_index("batch")
    n_seq = lax.axis_size("seq")
    n_batch = lax.axis_size("batch")
    swap = [(0, 1), (1, 0)]

    halves = 2
    half = rows // halves
    other_hidden = []
    for i in range(halves):
        other_hidden.append(lax.ppermute(image_hidden[:, i * half : (i + 1) * half], "head", swap))

    text = jnp.stack([text_keys, text_values], 1)
    t_rows = text.shape[2]
    text = text.reshape(prompts, 2, t_rows, heads, head_dim).transpose(0, 3, 1, 2, 4)
    text = jnp.pad(text, ((0, 0), (0, SLOTS - heads), (0, 0), (0, 0), (0, 0)))
    text = text.reshape(n_seq, 2, t_rows, head_dim)
    text = lax.all_to_all(text, "seq", split_axis=0, concat_axis=0, tiled=True)
    text_k = text[:, 0].reshape(n_seq * t_rows, head_dim)
    text_v = text[:, 1].reshape(n_seq * t_rows, head_dim).T

    n_y = n_seq // 4
    y_seat = seat // 4
    share = channels // (n_batch * n_y)
    piece = lax.dynamic_slice(
        out_weight,
        ((batch_seat * n_y + y_seat) * share, (1 - head_seat) * width_part),
        (share, width_part),
    )
    piece = lax.ppermute(piece, "head", swap)

    seats = jnp.arange(n_seq, dtype=jnp.int32)
    own_band = jnp.sum(jnp.where(seats == seat, patch_of, 0))
    own_flag = jnp.sum(jnp.where(seats == seat, refresh, 0))
    raster = own_band * rows + jnp.arange(rows, dtype=jnp.int32)
    cos, sin = rotary_tables(raster, head_dim, GRID_W)
    info = jnp.stack([head_seat.astype(jnp.int32), own_flag.astype(jnp.int32)])
    mod_view = modulation.transpose(1, 0, 2)
    weight_view = qkv_weight.transpose(1, 0, 2)
    gains = jnp.stack([q_gain, k_gain])
    send, fresh, got = [], [], []
    for i in range(halves):
        s, f = qkv(
            i,
            info,
            image_hidden,
            other_hidden[i],
            mod_view,
            weight_view,
            gains,
            cos,
            sin,
            stale_keys,
            stale_values,
        )
        send.append(s)
        fresh.append(f)
        got.append(
            lax.all_to_all(
                s.reshape(n_seq, 3, half, head_dim), "seq", split_axis=0, concat_axis=0, tiled=True
            )
        )
    piece, _ = lax.optimization_barrier((piece, send[0]))
    w_y = jnp.zeros((n_y, share, width_part), BF16)
    w_y = lax.dynamic_update_slice(w_y, piece[None], (y_seat, 0, 0))
    for d in range(1, n_y):
        moved = lax.ppermute(piece, "seq", [(i, (i + 4 * d) % n_seq) for i in range(n_seq)])
        w_y = lax.dynamic_update_slice(w_y, moved[None], ((y_seat - d) % n_y, 0, 0))
    w_y, _ = lax.optimization_barrier((w_y, send[1]))
    w_oth = jnp.zeros((n_batch, n_y, share, width_part), BF16)
    w_oth = lax.dynamic_update_slice(w_oth, w_y[None], (batch_seat, 0, 0, 0))
    for d in range(1, n_batch):
        moved = lax.ppermute(w_y, "batch", [(i, (i + d) % n_batch) for i in range(n_batch)])
        w_oth = lax.dynamic_update_slice(w_oth, moved[None], ((batch_seat - d) % n_batch, 0, 0, 0))
    w_oth = w_oth.reshape(channels, width_part)
    near = diag(send, fresh)
    got[1], near_sent = lax.optimization_barrier((got[1], near))
    far = lax.ppermute(near_sent, "head", swap)
    unit_prompt = jnp.minimum(seat // SLOTS, prompts - 1)
    length = jnp.sum(jnp.where(jnp.arange(prompts) == unit_prompt, text_len, 0)).astype(jnp.int32)
    back = attend(length[None], got, text_k, text_v)
    back = lax.all_to_all(
        back.reshape(n_seq * 2, 144, rows), ("seq", "head"), split_axis=0, concat_axis=0, tiled=True
    )
    gate = lax.dynamic_slice_in_dim(modulation[:, 2:3], head_seat * width_part, width_part, 2)
    return project(info, back, near, far, out_weight, w_oth, gate, image_hidden, cached_residual)


def solution(mesh):
    in_specs = (
        P("batch", "seq", "head"),
        P("batch", None, None),
        P(None, None, "head"),
        P("head", None),
        P(),
        P(),
        P("batch", "seq", "head"),
        P("batch", "seq", "head"),
        P("batch", "seq", "head"),
        P("batch", "seq", "head"),
        P("batch", "seq", "head"),
        P("batch"),
        P("batch"),
        P("batch"),
    )
    out_specs = P("batch", "seq", "head")
    return jax.shard_map(
        per_device, mesh=mesh, in_specs=in_specs, out_specs=out_specs, check_vma=False
    )
```

```python
import jax
import jax.numpy as jnp
from jax import lax
from jax.experimental import pallas as pl
from jax.experimental.pallas import tpu as pltpu
from jax.sharding import PartitionSpec as P


GRID_W = 64
EPS = 1e-06
LOG2E = 1.4426950408889634
F32 = jnp.float32
BF16 = jnp.bfloat16
NEG = -1e30
VMEM = 56 * 1024 * 1024
SLOTS = 8


def rotary_tables(raster, head_dim, grid_width):
    half_dim = head_dim // 2
    first_pairs = head_dim // 16
    axis_pairs = (half_dim - first_pairs) // 2
    pair_index = jnp.arange(half_dim, dtype=jnp.int32)
    pair_local = jnp.where(
        pair_index < first_pairs + axis_pairs,
        pair_index - first_pairs,
        pair_index - first_pairs - axis_pairs,
    )
    exponent = -pair_local.astype(F32) / float(axis_pairs)
    frequency = jnp.where(pair_index < first_pairs, F32(0.0), jnp.power(F32(10000.0), exponent))
    row_pos = (raster // grid_width).astype(F32)
    col_pos = (raster % grid_width).astype(F32)
    position = jnp.where(
        pair_index[None, :] < first_pairs + axis_pairs, row_pos[:, None], col_pos[:, None]
    )
    angles = position * frequency[None, :]
    cosine = jnp.cos(angles)
    sine = jnp.sin(angles)
    return (jnp.concatenate([cosine, cosine], axis=-1), jnp.concatenate([-sine, sine], axis=-1))


def qkv_body(
    info, own, oth, mod_own, mod_oth, w_own, w_oth, gains, cos, sin, stale_k, stale_v, send, fresh, mod_s, wide_s
):
    n = pl.program_id(0)
    prompts, rows, part = own.shape
    width = 2 * part
    tile = 16

    @pl.when(n == 0)
    def _():
        for p in range(prompts):
            for k in range(2):
                for m, mod in enumerate((mod_own, mod_oth)):
                    row = mod[k, p : p + 1, :] + float(k)
                    wide_s[k, :, m * part : (m + 1) * part] = jnp.broadcast_to(row, (8, part))

            def norm(i, c):
                at = pl.multiple_of(i * tile, tile)
                a = own[p, pl.ds(at, tile), :].astype(F32)
                b = oth[p, pl.ds(at, tile), :].astype(F32)
                mean = (jnp.sum(a, -1, keepdims=True) + jnp.sum(b, -1, keepdims=True)) / width
                a, b = a - mean, b - mean
                var = (jnp.sum(a * a, -1, keepdims=True) + jnp.sum(b * b, -1, keepdims=True)) / width
                inv = lax.rsqrt(var + EPS)
                a = moved(a * inv, 0)
                b = moved(b * inv, part)
                to = pl.multiple_of(p * rows + i * tile, tile)
                mod_s[pl.ds(to, tile), 0:part] = a.astype(BF16)
                mod_s[pl.ds(to, tile), part:width] = b.astype(BF16)
                return c

            def moved(x, at):
                shift, scale = (wide_s[k, :, at : at + part] for k in range(2))
                parts = [x[r : r + 8] * scale + shift for r in range(0, tile, 8)]
                return jnp.concatenate(parts, 0)

            lax.fori_loop(0, rows // tile, norm, 0, unroll=4)

    heads = w_own.shape[2] // 128
    per = 2
    flag = info[1]

    def products():
        for j in range(0, heads, per):
            cols = slice(j * 128, (j + per) * 128)
            acc = jnp.dot(mod_s[:, 0:part], w_own[0, :, cols], preferred_element_type=F32)
            acc = acc + jnp.dot(mod_s[:, part:width], w_oth[0, :, cols], preferred_element_type=F32)
            for p in range(prompts):
                for e in range(per):
                    yield p, j + e, acc[p * rows : (p + 1) * rows, e * 128 : (e + 1) * 128]

    def turned(x, gain):
        x = x * lax.rsqrt(jnp.mean(x * x, axis=-1, keepdims=True) + EPS) * gain
        return x * cos[...] + pltpu.roll(x, 64, 1) * sin[...]

    @pl.when(n == 0)
    def _():
        for p, j, x in products():
            send[p, j, 0] = turned(x, gains[0:1, :]).astype(BF16)

    @pl.when(n == 1)
    def _():
        for p, j, x in products():
            new = turned(x, gains[1:2, :]).astype(BF16)
            fresh[p, j, 0] = new
            send[p, j, 0] = jnp.where(flag == 1, new, stale_k[p, :, j * 128 : (j + 1) * 128])

    @pl.when(n == 2)
    def _():
        for p, j, x in products():
            new = x.astype(BF16)
            used = jnp.where(flag == 1, new, stale_v[p, :, j * 128 : (j + 1) * 128])
            for r in range(0, rows, 128):
                fresh[p, j, 0, r : r + 128, :] = jnp.transpose(new[r : r + 128, :])
                send[p, j, 0, r : r + 128, :] = jnp.transpose(used[r : r + 128, :])


def qkv(c, info, own, oth, modulation, w, gains, cos, sin, stale_k, stale_v):
    prompts, rows, part = oth.shape
    channels = stale_k.shape[2]
    heads = channels // 128
    whole = lambda *shape: pl.BlockSpec(shape, lambda n, s: (0,) * len(shape))
    half = lambda *shape: pl.BlockSpec(shape, lambda n, s: (0, c, 0))
    return pl.pallas_call(
        qkv_body,
        grid_spec=pltpu.PrefetchScalarGridSpec(
            num_scalar_prefetch=1,
            grid=(3,),
            in_specs=[
                half(prompts, rows, part),
                whole(prompts, rows, part),
                pl.BlockSpec((3, prompts, part), lambda n, s: (0, 0, s[0])),
                pl.BlockSpec((3, prompts, part), lambda n, s: (0, 0, 1 - s[0])),
                pl.BlockSpec((1, part, channels), lambda n, s: (n, s[0], 0)),
                pl.BlockSpec((1, part, channels), lambda n, s: (n, 1 - s[0], 0)),
                whole(2, 128),
                pl.BlockSpec((rows, 128), lambda n, s: (c, 0)),
                pl.BlockSpec((rows, 128), lambda n, s: (c, 0)),
                half(prompts, rows, channels),
                half(prompts, rows, channels),
            ],
            out_specs=[
                pl.BlockSpec((prompts, SLOTS, 1, rows, 128), lambda n, s: (0, 0, n, 0, 0)),
                pl.BlockSpec(
                    (prompts, heads, 1, rows, 128), lambda n, s: (0, 0, jnp.maximum(n - 1, 0), 0, 0)
                ),
            ],
            scratch_shapes=[
                pltpu.VMEM((prompts * rows, 2 * part), BF16),
                pltpu.VMEM((2, 8, 2 * part), F32),
            ],
        ),
        out_shape=[
            jax.ShapeDtypeStruct((prompts, SLOTS, 3, rows, 128), BF16),
            jax.ShapeDtypeStruct((prompts, heads, 2, rows, 128), BF16),
        ],
        compiler_params=pltpu.CompilerParams(
            dimension_semantics=("arbitrary",), vmem_limit_bytes=VMEM
        ),
        cost_estimate=pl.CostEstimate(
            flops=2 * prompts * rows * 2 * part * 3 * channels, bytes_accessed=20_000_000, transcendentals=0
        ),
        name="qkv",
    )(info, own, oth, modulation, modulation, w, w, gains, cos, sin, stale_k, stale_v)


CONTRACT = (((1,), (1,)), ((), ()))


def log_sum_rows(lse):
    lse = jnp.broadcast_to(lse, (16, lse.shape[1]))
    first = lse.astype(BF16).astype(F32)
    second = (lse - first).astype(BF16).astype(F32)
    third = lse - first - second
    at = lax.broadcasted_iota(jnp.int32, lse.shape, 0)
    return jnp.where(at == 0, first, jnp.where(at == 1, second, third)).astype(BF16)


def diag_body(*refs):
    halves = len(refs) // 2
    send, fresh, out = refs[:halves], refs[halves : 2 * halves], refs[-1]
    c = 128**-0.5 * LOG2E
    for e in range(out.shape[1]):
        q = jnp.concatenate([r[0, e, 0] for r in send], 0)
        k = jnp.concatenate([r[0, e, 0] for r in fresh], 0)
        v = jnp.concatenate([r[0, e, 1] for r in fresh], 1)
        s = lax.dot_general(k, q, CONTRACT, preferred_element_type=F32) * c
        top = jnp.max(s, axis=0, keepdims=True)
        w = jnp.exp2(s - top)
        total = jnp.sum(w, axis=0, keepdims=True)
        o = jnp.dot(v, w.astype(BF16), preferred_element_type=F32)
        out[0, e, 0:128, :] = (o / total).astype(BF16)
        out[0, e, 128:144, :] = log_sum_rows(top + jnp.log2(total))


def diag(send, fresh):
    prompts, heads, _, part, _ = fresh[0].shape
    rows = part * len(send)
    return pl.pallas_call(
        diag_body,
        grid=(prompts,),
        in_specs=[pl.BlockSpec((1, heads, 1, part, 128), lambda p: (p, 0, 0, 0, 0))] * len(send)
        + [pl.BlockSpec((1, heads, 2, part, 128), lambda p: (p, 0, 0, 0, 0))] * len(send),
        out_specs=pl.BlockSpec((1, heads, 144, rows), lambda p: (p, 0, 0, 0)),
        out_shape=jax.ShapeDtypeStruct((prompts, heads, 144, rows), BF16),
        compiler_params=pltpu.CompilerParams(
            dimension_semantics=("arbitrary",), vmem_limit_bytes=VMEM
        ),
        cost_estimate=pl.CostEstimate(
            flops=4 * prompts * heads * rows * rows * 128,
            bytes_accessed=4_000_000,
            transcendentals=prompts * heads * rows * rows,
        ),
        name="diag",
    )(*send, *fresh)


def attend_body(info, got_0, got_1, text_k, text_v, out, s_even, s_odd, top_s):
    g = pl.program_id(0)
    got = (got_0, got_1)
    blocks = got_0.shape[0]
    rows = 2 * got_0.shape[2]
    c = 128**-0.5 * LOG2E
    lead = text_k.shape[0] // rows
    tiles = lead + blocks - 1
    groups = [list(range(i, min(i + 4, tiles))) for i in range(0, tiles, 4)]
    if len(groups[-1]) == 1:
        last = groups.pop()
        groups[-1] = groups[-1] + last

    def block_of(b, i):
        return lax.rem(b + 1 + (i - lead), blocks)

    def keys(b, i):
        if i < lead:
            return [text_k[i * rows : (i + 1) * rows, :]]
        return [r[block_of(b, i), 1] for r in got]

    def values(b, i):
        if i < lead:
            return [text_v[:, i * rows : (i + 1) * rows]]
        return [r[block_of(b, i), 2] for r in got]

    def queries(b):
        q = jnp.concatenate([r[b, 0] for r in got], 0).astype(F32) * c
        high = q.astype(BF16)
        return jnp.concatenate([high, (q - high.astype(F32)).astype(BF16)], 1)

    def score(b, q, group, top, s_ref):
        k = jnp.concatenate([x for i in group for x in keys(b, i)], 0)
        scores = lax.dot_general(jnp.concatenate([k, k], 1), q, CONTRACT, preferred_element_type=F32)
        for m, i in enumerate(group):
            s = scores[m * rows : (m + 1) * rows, :]
            if i < lead:
                at = i * rows + lax.broadcasted_iota(jnp.int32, s.shape, 0)
                s = jnp.where(at < info[0], s, NEG)
            s_ref[i] = s
            part = jnp.max(s.reshape(rows // 8, 8, rows), axis=0)
            top = part if top is None else jnp.maximum(top, part)
        return top

    def whole_top(top):
        return jnp.broadcast_to(jnp.max(top, axis=0, keepdims=True), (8, rows))

    @pl.when(g == 0)
    def _():
        top = None
        q = queries(0)
        for group in groups:
            top = score(0, q, group, top, s_even)
        top_s[...] = whole_top(top)

    top = top_s[...]
    for k in range(2):
        b = 2 * g + k
        nxt = lax.rem(b + 1, blocks)
        here, there = (s_even, s_odd) if k == 0 else (s_odd, s_even)
        total = None
        acc = None
        nxt_top = None
        late = None
        q = queries(nxt)

        def product(acc, late):
            group, w = late
            v = jnp.concatenate([x for i in group for x in values(b, i)], 1)
            o = jnp.dot(v, w, preferred_element_type=F32)
            return o if acc is None else acc + o

        for group in groups:
            nxt_top = score(nxt, q, group, nxt_top, there)
            w = []
            for i in group:
                x = jnp.exp2(here[i].reshape(rows // 8, 8, rows) - top[None])
                part = jnp.sum(x, axis=0)
                total = part if total is None else total + part
                w.append(x.reshape(rows, rows).astype(BF16))
            if late is not None:
                acc = product(acc, late)
            late = (group, jnp.concatenate(w, 0))
        acc = product(acc, late)
        total = jnp.sum(total, axis=0, keepdims=True)
        acc = (acc / total).astype(BF16)
        lse = log_sum_rows(top[0:1, :] + jnp.log2(total))
        for seat in range(2):
            out[k, seat, 0:128, :] = acc
            out[k, seat, 128:144, :] = lse
        top = whole_top(nxt_top)
    top_s[...] = top


def attend(info, got, text_k, text_v):
    blocks, _, part, _ = got[0].shape
    rows = part * len(got)
    tiles = text_k.shape[0] // rows + blocks - 1
    return pl.pallas_call(
        attend_body,
        grid_spec=pltpu.PrefetchScalarGridSpec(
            num_scalar_prefetch=1,
            grid=(blocks // 2,),
            in_specs=[
                pl.BlockSpec(got[0].shape, lambda b, s: (0, 0, 0, 0)),
                pl.BlockSpec(got[1].shape, lambda b, s: (0, 0, 0, 0)),
                pl.BlockSpec(text_k.shape, lambda b, s: (0, 0)),
                pl.BlockSpec(text_v.shape, lambda b, s: (0, 0)),
            ],
            out_specs=pl.BlockSpec((2, 2, 144, rows), lambda b, s: (b, 0, 0, 0)),
            scratch_shapes=[
                pltpu.VMEM((tiles, rows, rows), F32),
                pltpu.VMEM((tiles, rows, rows), F32),
                pltpu.VMEM((8, rows), F32),
            ],
        ),
        out_shape=jax.ShapeDtypeStruct((blocks, 2, 144, rows), BF16),
        compiler_params=pltpu.CompilerParams(
            dimension_semantics=("arbitrary",), vmem_limit_bytes=VMEM
        ),
        cost_estimate=pl.CostEstimate(
            flops=4 * blocks * rows * tiles * rows * 128 * 2,
            bytes_accessed=8_000_000,
            transcendentals=blocks * rows * tiles * rows,
        ),
        name="attend",
    )(info, *got, text_k, text_v)


def project_body(info, got, near, far, w_own, w_oth, gate, hidden, cached, out, all_s):
    n = pl.program_id(0)
    prompts, rows, _ = hidden.shape
    part = w_own.shape[0]
    heads = part // 128
    h = info[0]

    def log_sum(x):
        x = x.astype(F32)
        return x[0:1, :] + x[1:2, :] + x[2:3, :]

    @pl.when(n == 0)
    def _():
        for p in range(prompts):
            for k in range(2):
                own = (near, far)[k]
                seat = h if k == 0 else 1 - h
                for j in range(heads):
                    at = (p * SLOTS + j) * 2 + seat
                    a = log_sum(got[at, 128:144, :])
                    b = log_sum(own[p, j, 128:144, :])
                    high = jnp.maximum(a, b)
                    a, b = jnp.exp2(a - high), jnp.exp2(b - high)
                    o = (got[at, 0:128, :].astype(F32) * a + own[p, j, 0:128, :].astype(F32) * b) / (a + b)
                    col = (k * heads + j) * 128
                    all_s[p * rows : (p + 1) * rows, col : col + 128] = jnp.transpose(o.astype(BF16))

    acc = jnp.dot(all_s[:, 0:part], w_own[...], preferred_element_type=F32)
    acc = acc + jnp.dot(all_s[:, part : 2 * part], w_oth[...], preferred_element_type=F32)
    for p in range(prompts):
        y = hidden[p].astype(F32) + gate[p] * acc[p * rows : (p + 1) * rows, :]
        out[p] = (y + cached[p].astype(F32)).astype(BF16)


def project(info, got, near, far, w_out, w_oth, gate, hidden, cached):
    prompts, rows, width = hidden.shape
    part = w_out.shape[0]
    bn = 512
    steps = width // bn
    return pl.pallas_call(
        project_body,
        grid_spec=pltpu.PrefetchScalarGridSpec(
            num_scalar_prefetch=1,
            grid=(steps,),
            in_specs=[
                pl.BlockSpec(got.shape, lambda n, s: (0, 0, 0)),
                pl.BlockSpec(near.shape, lambda n, s: (0, 0, 0, 0)),
                pl.BlockSpec(far.shape, lambda n, s: (0, 0, 0, 0)),
                pl.BlockSpec((part, bn), lambda n, s: (0, s[0] * steps + n)),
                pl.BlockSpec((part, bn), lambda n, s: (0, n)),
                pl.BlockSpec((prompts, 1, bn), lambda n, s: (0, 0, n)),
                pl.BlockSpec((prompts, rows, bn), lambda n, s: (0, 0, n)),
                pl.BlockSpec((prompts, rows, bn), lambda n, s: (0, 0, n)),
            ],
            out_specs=pl.BlockSpec((prompts, rows, bn), lambda n, s: (0, 0, n)),
            scratch_shapes=[pltpu.VMEM((prompts * rows, 2 * part), BF16)],
        ),
        out_shape=jax.ShapeDtypeStruct((prompts, rows, width), BF16),
        compiler_params=pltpu.CompilerParams(
            dimension_semantics=("arbitrary",), vmem_limit_bytes=VMEM
        ),
        cost_estimate=pl.CostEstimate(
            flops=4 * prompts * rows * part * width, bytes_accessed=12_000_000, transcendentals=0
        ),
        name="project",
    )(info, got, near, far, w_out, w_oth, gate, hidden, cached)


def per_device(
    image_hidden,
    modulation,
    qkv_weight,
    out_weight,
    q_gain,
    k_gain,
    text_keys,
    text_values,
    stale_keys,
    stale_values,
    cached_residual,
    patch_of,
    refresh,
    text_len,
):
    prompts, rows, width_part = image_hidden.shape
    head_dim = q_gain.shape[0]
    channels = out_weight.shape[0]
    heads = channels // head_dim
    seat = lax.axis_index("seq")
    head_seat = lax.axis_index("head")
    batch_seat = lax.axis_index("batch")
    n_seq = lax.axis_size("seq")
    n_batch = lax.axis_size("batch")
    swap = [(0, 1), (1, 0)]

    halves = 2
    half = rows // halves
    other_hidden = []
    for i in range(halves):
        other_hidden.append(lax.ppermute(image_hidden[:, i * half : (i + 1) * half], "head", swap))

    text = jnp.stack([text_keys, text_values], 1)
    t_rows = text.shape[2]
    text = text.reshape(prompts, 2, t_rows, heads, head_dim).transpose(0, 3, 1, 2, 4)
    text = jnp.pad(text, ((0, 0), (0, SLOTS - heads), (0, 0), (0, 0), (0, 0)))
    text = text.reshape(n_seq, 2, t_rows, head_dim)
    text = lax.all_to_all(text, "seq", split_axis=0, concat_axis=0, tiled=True)
    text_k = text[:, 0].reshape(n_seq * t_rows, head_dim)
    text_v = text[:, 1].reshape(n_seq * t_rows, head_dim).T

    n_y = n_seq // 4
    y_seat = seat // 4
    share = channels // (n_batch * n_y)
    piece = lax.dynamic_slice(
        out_weight,
        ((batch_seat * n_y + y_seat) * share, (1 - head_seat) * width_part),
        (share, width_part),
    )
    piece = lax.ppermute(piece, "head", swap)

    seats = jnp.arange(n_seq, dtype=jnp.int32)
    own_band = jnp.sum(jnp.where(seats == seat, patch_of, 0))
    own_flag = jnp.sum(jnp.where(seats == seat, refresh, 0))
    raster = own_band * rows + jnp.arange(rows, dtype=jnp.int32)
    cos, sin = rotary_tables(raster, head_dim, GRID_W)
    info = jnp.stack([head_seat.astype(jnp.int32), own_flag.astype(jnp.int32)])
    mod_view = modulation.transpose(1, 0, 2)
    weight_view = qkv_weight.transpose(1, 0, 2)
    gains = jnp.stack([q_gain, k_gain])
    send, fresh, got = [], [], []
    for i in range(halves):
        s, f = qkv(
            i,
            info,
            image_hidden,
            other_hidden[i],
            mod_view,
            weight_view,
            gains,
            cos,
            sin,
            stale_keys,
            stale_values,
        )
        send.append(s)
        fresh.append(f)
        got.append(
            lax.all_to_all(
                s.reshape(n_seq, 3, half, head_dim), "seq", split_axis=0, concat_axis=0, tiled=True
            )
        )
    piece, _ = lax.optimization_barrier((piece, send[0]))
    w_y = jnp.zeros((n_y, share, width_part), BF16)
    w_y = lax.dynamic_update_slice(w_y, piece[None], (y_seat, 0, 0))
    for d in range(1, n_y):
        moved = lax.ppermute(piece, "seq", [(i, (i + 4 * d) % n_seq) for i in range(n_seq)])
        w_y = lax.dynamic_update_slice(w_y, moved[None], ((y_seat - d) % n_y, 0, 0))
    w_y, _ = lax.optimization_barrier((w_y, send[1]))
    w_oth = jnp.zeros((n_batch, n_y, share, width_part), BF16)
    w_oth = lax.dynamic_update_slice(w_oth, w_y[None], (batch_seat, 0, 0, 0))
    for d in range(1, n_batch):
        moved = lax.ppermute(w_y, "batch", [(i, (i + d) % n_batch) for i in range(n_batch)])
        w_oth = lax.dynamic_update_slice(w_oth, moved[None], ((batch_seat - d) % n_batch, 0, 0, 0))
    w_oth = w_oth.reshape(channels, width_part)
    near = diag(send, fresh)
    got[1], near_sent = lax.optimization_barrier((got[1], near))
    far = lax.ppermute(near_sent, "head", swap)
    unit_prompt = jnp.minimum(seat // SLOTS, prompts - 1)
    length = jnp.sum(jnp.where(jnp.arange(prompts) == unit_prompt, text_len, 0)).astype(jnp.int32)
    back = attend(length[None], got, text_k, text_v)
    back = lax.all_to_all(
        back.reshape(n_seq * 2, 144, rows), ("seq", "head"), split_axis=0, concat_axis=0, tiled=True
    )
    gate = lax.dynamic_slice_in_dim(modulation[:, 2:3], head_seat * width_part, width_part, 2)
    return project(info, back, near, far, out_weight, w_oth, gate, image_hidden, cached_residual)


def solution(mesh):
    in_specs = (
        P("batch", "seq", "head"),
        P("batch", None, None),
        P(None, None, "head"),
        P("head", None),
        P(),
        P(),
        P("batch", "seq", "head"),
        P("batch", "seq", "head"),
        P("batch", "seq", "head"),
        P("batch", "seq", "head"),
        P("batch", "seq", "head"),
        P("batch"),
        P("batch"),
        P("batch"),
    )
    out_specs = P("batch", "seq", "head")
    return jax.shard_map(
        per_device, mesh=mesh, in_specs=in_specs, out_specs=out_specs, check_vma=False
    )
```

```python
import jax
import jax.numpy as jnp
from jax import lax
from jax.experimental import pallas as pl
from jax.experimental.pallas import tpu as pltpu
from jax.sharding import PartitionSpec as P


GRID_W = 64
EPS = 1e-06
LOG2E = 1.4426950408889634
F32 = jnp.float32
BF16 = jnp.bfloat16
NEG = -1e30
VMEM = 56 * 1024 * 1024
SLOTS = 8


def rotary_tables(raster, head_dim, grid_width):
    half_dim = head_dim // 2
    first_pairs = head_dim // 16
    axis_pairs = (half_dim - first_pairs) // 2
    pair_index = jnp.arange(half_dim, dtype=jnp.int32)
    pair_local = jnp.where(
        pair_index < first_pairs + axis_pairs,
        pair_index - first_pairs,
        pair_index - first_pairs - axis_pairs,
    )
    exponent = -pair_local.astype(F32) / float(axis_pairs)
    frequency = jnp.where(pair_index < first_pairs, F32(0.0), jnp.power(F32(10000.0), exponent))
    row_pos = (raster // grid_width).astype(F32)
    col_pos = (raster % grid_width).astype(F32)
    position = jnp.where(
        pair_index[None, :] < first_pairs + axis_pairs, row_pos[:, None], col_pos[:, None]
    )
    angles = position * frequency[None, :]
    cosine = jnp.cos(angles)
    sine = jnp.sin(angles)
    return (jnp.concatenate([cosine, cosine], axis=-1), jnp.concatenate([-sine, sine], axis=-1))


def qkv_body(
    info, own, oth, mod_own, mod_oth, w_own, w_oth, gains, cos, sin, stale_k, stale_v, send, fresh, mod_s, wide_s
):
    n = pl.program_id(0)
    prompts, rows, part = own.shape
    width = 2 * part
    tile = 16

    @pl.when(n == 0)
    def _():
        for p in range(prompts):
            for k in range(2):
                for m, mod in enumerate((mod_own, mod_oth)):
                    row = mod[k, p : p + 1, :] + float(k)
                    wide_s[k, :, m * part : (m + 1) * part] = jnp.broadcast_to(row, (8, part))

            def norm(i, c):
                at = pl.multiple_of(i * tile, tile)
                a = own[p, pl.ds(at, tile), :].astype(F32)
                b = oth[p, pl.ds(at, tile), :].astype(F32)
                mean = (jnp.sum(a, -1, keepdims=True) + jnp.sum(b, -1, keepdims=True)) / width
                a, b = a - mean, b - mean
                var = (jnp.sum(a * a, -1, keepdims=True) + jnp.sum(b * b, -1, keepdims=True)) / width
                inv = lax.rsqrt(var + EPS)
                a = moved(a * inv, 0)
                b = moved(b * inv, part)
                to = pl.multiple_of(p * rows + i * tile, tile)
                mod_s[pl.ds(to, tile), 0:part] = a.astype(BF16)
                mod_s[pl.ds(to, tile), part:width] = b.astype(BF16)
                return c

            def moved(x, at):
                shift, scale = (wide_s[k, :, at : at + part] for k in range(2))
                parts = [x[r : r + 8] * scale + shift for r in range(0, tile, 8)]
                return jnp.concatenate(parts, 0)

            lax.fori_loop(0, rows // tile, norm, 0, unroll=4)

    heads = w_own.shape[2] // 128
    per = 2
    flag = info[1]

    def products():
        for j in range(0, heads, per):
            cols = slice(j * 128, (j + per) * 128)
            acc = jnp.dot(mod_s[:, 0:part], w_own[0, :, cols], preferred_element_type=F32)
            acc = acc + jnp.dot(mod_s[:, part:width], w_oth[0, :, cols], preferred_element_type=F32)
            for p in range(prompts):
                for e in range(per):
                    yield p, j + e, acc[p * rows : (p + 1) * rows, e * 128 : (e + 1) * 128]

    def turned(x, gain):
        x = x * lax.rsqrt(jnp.mean(x * x, axis=-1, keepdims=True) + EPS) * gain
        return x * cos[...] + pltpu.roll(x, 64, 1) * sin[...]

    @pl.when(n == 0)
    def _():
        for p, j, x in products():
            send[p, j, 0] = turned(x, gains[0:1, :]).astype(BF16)

    @pl.when(n == 1)
    def _():
        for p, j, x in products():
            new = turned(x, gains[1:2, :]).astype(BF16)
            fresh[p, j, 0] = new
            send[p, j, 0] = jnp.where(flag == 1, new, stale_k[p, :, j * 128 : (j + 1) * 128])

    @pl.when(n == 2)
    def _():
        for p, j, x in products():
            new = x.astype(BF16)
            used = jnp.where(flag == 1, new, stale_v[p, :, j * 128 : (j + 1) * 128])
            for r in range(0, rows, 128):
                fresh[p, j, 0, r : r + 128, :] = jnp.transpose(new[r : r + 128, :])
                send[p, j, 0, r : r + 128, :] = jnp.transpose(used[r : r + 128, :])


def qkv(c, info, own, oth, modulation, w, gains, cos, sin, stale_k, stale_v):
    prompts, rows, part = oth.shape
    channels = stale_k.shape[2]
    heads = channels // 128
    whole = lambda *shape: pl.BlockSpec(shape, lambda n, s: (0,) * len(shape))
    half = lambda *shape: pl.BlockSpec(shape, lambda n, s: (0, c, 0))
    return pl.pallas_call(
        qkv_body,
        grid_spec=pltpu.PrefetchScalarGridSpec(
            num_scalar_prefetch=1,
            grid=(3,),
            in_specs=[
                half(prompts, rows, part),
                whole(prompts, rows, part),
                pl.BlockSpec((3, prompts, part), lambda n, s: (0, 0, s[0])),
                pl.BlockSpec((3, prompts, part), lambda n, s: (0, 0, 1 - s[0])),
                pl.BlockSpec((1, part, channels), lambda n, s: (n, s[0], 0)),
                pl.BlockSpec((1, part, channels), lambda n, s: (n, 1 - s[0], 0)),
                whole(2, 128),
                pl.BlockSpec((rows, 128), lambda n, s: (c, 0)),
                pl.BlockSpec((rows, 128), lambda n, s: (c, 0)),
                half(prompts, rows, channels),
                half(prompts, rows, channels),
            ],
            out_specs=[
                pl.BlockSpec((prompts, SLOTS, 1, rows, 128), lambda n, s: (0, 0, n, 0, 0)),
                pl.BlockSpec(
                    (prompts, heads, 1, rows, 128), lambda n, s: (0, 0, jnp.maximum(n - 1, 0), 0, 0)
                ),
            ],
            scratch_shapes=[
                pltpu.VMEM((prompts * rows, 2 * part), BF16),
                pltpu.VMEM((2, 8, 2 * part), F32),
            ],
        ),
        out_shape=[
            jax.ShapeDtypeStruct((prompts, SLOTS, 3, rows, 128), BF16),
            jax.ShapeDtypeStruct((prompts, heads, 2, rows, 128), BF16),
        ],
        compiler_params=pltpu.CompilerParams(
            dimension_semantics=("arbitrary",), vmem_limit_bytes=VMEM
        ),
        cost_estimate=pl.CostEstimate(
            flops=2 * prompts * rows * 2 * part * 3 * channels, bytes_accessed=20_000_000, transcendentals=0
        ),
        name="qkv",
    )(info, own, oth, modulation, modulation, w, w, gains, cos, sin, stale_k, stale_v)


CONTRACT = (((1,), (1,)), ((), ()))


def log_sum_rows(lse):
    lse = jnp.broadcast_to(lse, (16, lse.shape[1]))
    first = lse.astype(BF16).astype(F32)
    second = (lse - first).astype(BF16).astype(F32)
    third = lse - first - second
    at = lax.broadcasted_iota(jnp.int32, lse.shape, 0)
    return jnp.where(at == 0, first, jnp.where(at == 1, second, third)).astype(BF16)


def diag_body(*refs):
    halves = len(refs) // 2
    send, fresh, out = refs[:halves], refs[halves : 2 * halves], refs[-1]
    c = 128**-0.5 * LOG2E
    for e in range(out.shape[1]):
        q = jnp.concatenate([r[0, e, 0] for r in send], 0)
        k = jnp.concatenate([r[0, e, 0] for r in fresh], 0)
        v = jnp.concatenate([r[0, e, 1] for r in fresh], 1)
        s = lax.dot_general(k, q, CONTRACT, preferred_element_type=F32) * c
        top = jnp.max(s, axis=0, keepdims=True)
        w = jnp.exp2(s - top)
        total = jnp.sum(w, axis=0, keepdims=True)
        o = jnp.dot(v, w.astype(BF16), preferred_element_type=F32)
        out[0, e, 0:128, :] = (o / total).astype(BF16)
        out[0, e, 128:144, :] = log_sum_rows(top + jnp.log2(total))


def diag(send, fresh):
    prompts, heads, _, part, _ = fresh[0].shape
    rows = part * len(send)
    return pl.pallas_call(
        diag_body,
        grid=(prompts,),
        in_specs=[pl.BlockSpec((1, heads, 1, part, 128), lambda p: (p, 0, 0, 0, 0))] * len(send)
        + [pl.BlockSpec((1, heads, 2, part, 128), lambda p: (p, 0, 0, 0, 0))] * len(send),
        out_specs=pl.BlockSpec((1, heads, 144, rows), lambda p: (p, 0, 0, 0)),
        out_shape=jax.ShapeDtypeStruct((prompts, heads, 144, rows), BF16),
        compiler_params=pltpu.CompilerParams(
            dimension_semantics=("arbitrary",), vmem_limit_bytes=VMEM
        ),
        cost_estimate=pl.CostEstimate(
            flops=4 * prompts * heads * rows * rows * 128,
            bytes_accessed=4_000_000,
            transcendentals=prompts * heads * rows * rows,
        ),
        name="diag",
    )(*send, *fresh)


def attend_body(info, got_0, got_1, text_k, text_v, out, s_even, s_odd, top_s):
    g = pl.program_id(0)
    got = (got_0, got_1)
    blocks = got_0.shape[0]
    rows = 2 * got_0.shape[2]
    c = 128**-0.5 * LOG2E
    lead = text_k.shape[0] // rows
    tiles = lead + blocks - 1
    groups = [list(range(i, min(i + 4, tiles))) for i in range(0, tiles, 4)]
    if len(groups[-1]) == 1:
        last = groups.pop()
        groups[-1] = groups[-1] + last

    def block_of(b, i):
        return lax.rem(b + 1 + (i - lead), blocks)

    def keys(b, i):
        if i < lead:
            return [text_k[i * rows : (i + 1) * rows, :]]
        return [r[block_of(b, i), 1] for r in got]

    def values(b, i):
        if i < lead:
            return [text_v[:, i * rows : (i + 1) * rows]]
        return [r[block_of(b, i), 2] for r in got]

    def queries(b):
        q = jnp.concatenate([r[b, 0] for r in got], 0).astype(F32) * c
        high = q.astype(BF16)
        return jnp.concatenate([high, (q - high.astype(F32)).astype(BF16)], 1)

    def score(b, q, group, top, s_ref):
        k = jnp.concatenate([x for i in group for x in keys(b, i)], 0)
        scores = lax.dot_general(jnp.concatenate([k, k], 1), q, CONTRACT, preferred_element_type=F32)
        for m, i in enumerate(group):
            s = scores[m * rows : (m + 1) * rows, :]
            if i < lead:
                at = i * rows + lax.broadcasted_iota(jnp.int32, s.shape, 0)
                s = jnp.where(at < info[0], s, NEG)
            s_ref[i] = s
            part = jnp.max(s.reshape(rows // 8, 8, rows), axis=0)
            top = part if top is None else jnp.maximum(top, part)
        return top

    def whole_top(top):
        return jnp.broadcast_to(jnp.max(top, axis=0, keepdims=True), (8, rows))

    @pl.when(g == 0)
    def _():
        top = None
        q = queries(0)
        for group in groups:
            top = score(0, q, group, top, s_even)
        top_s[...] = whole_top(top)

    top = top_s[...]
    for k in range(2):
        b = 2 * g + k
        nxt = lax.rem(b + 1, blocks)
        here, there = (s_even, s_odd) if k == 0 else (s_odd, s_even)
        total = None
        acc = None
        nxt_top = None
        late = None
        q = queries(nxt)

        def product(acc, late):
            group, w = late
            v = jnp.concatenate([x for i in group for x in values(b, i)], 1)
            o = jnp.dot(v, w, preferred_element_type=F32)
            return o if acc is None else acc + o

        for group in groups:
            nxt_top = score(nxt, q, group, nxt_top, there)
            w = []
            for i in group:
                x = jnp.exp2(here[i].reshape(rows // 8, 8, rows) - top[None])
                part = jnp.sum(x, axis=0)
                total = part if total is None else total + part
                w.append(x.reshape(rows, rows).astype(BF16))
            if late is not None:
                acc = product(acc, late)
            late = (group, jnp.concatenate(w, 0))
        acc = product(acc, late)
        total = jnp.sum(total, axis=0, keepdims=True)
        acc = (acc / total).astype(BF16)
        lse = log_sum_rows(top[0:1, :] + jnp.log2(total))
        for seat in range(2):
            out[k, seat, 0:128, :] = acc
            out[k, seat, 128:144, :] = lse
        top = whole_top(nxt_top)
    top_s[...] = top


def attend(info, got, text_k, text_v):
    blocks, _, part, _ = got[0].shape
    rows = part * len(got)
    tiles = text_k.shape[0] // rows + blocks - 1
    return pl.pallas_call(
        attend_body,
        grid_spec=pltpu.PrefetchScalarGridSpec(
            num_scalar_prefetch=1,
            grid=(blocks // 2,),
            in_specs=[
                pl.BlockSpec(got[0].shape, lambda b, s: (0, 0, 0, 0)),
                pl.BlockSpec(got[1].shape, lambda b, s: (0, 0, 0, 0)),
                pl.BlockSpec(text_k.shape, lambda b, s: (0, 0)),
                pl.BlockSpec(text_v.shape, lambda b, s: (0, 0)),
            ],
            out_specs=pl.BlockSpec((2, 2, 144, rows), lambda b, s: (b, 0, 0, 0)),
            scratch_shapes=[
                pltpu.VMEM((tiles, rows, rows), F32),
                pltpu.VMEM((tiles, rows, rows), F32),
                pltpu.VMEM((8, rows), F32),
            ],
        ),
        out_shape=jax.ShapeDtypeStruct((blocks, 2, 144, rows), BF16),
        compiler_params=pltpu.CompilerParams(
            dimension_semantics=("arbitrary",), vmem_limit_bytes=VMEM
        ),
        cost_estimate=pl.CostEstimate(
            flops=4 * blocks * rows * tiles * rows * 128 * 2,
            bytes_accessed=8_000_000,
            transcendentals=blocks * rows * tiles * rows,
        ),
        name="attend",
    )(info, *got, text_k, text_v)


def project_body(info, got, near, far, w_own, w_oth, gate, hidden, cached, out, all_s):
    n = pl.program_id(0)
    prompts, rows, _ = hidden.shape
    part = w_own.shape[0]
    heads = part // 128
    h = info[0]

    def log_sum(x):
        x = x.astype(F32)
        return x[0:1, :] + x[1:2, :] + x[2:3, :]

    @pl.when(n == 0)
    def _():
        for p in range(prompts):
            for k in range(2):
                own = (near, far)[k]
                seat = h if k == 0 else 1 - h
                for j in range(heads):
                    at = (p * SLOTS + j) * 2 + seat
                    a = log_sum(got[at, 128:144, :])
                    b = log_sum(own[p, j, 128:144, :])
                    high = jnp.maximum(a, b)
                    a, b = jnp.exp2(a - high), jnp.exp2(b - high)
                    shrink = 1.0 / (a + b)
                    a, b = a * shrink, b * shrink
                    o = got[at, 0:128, :].astype(F32) * a + own[p, j, 0:128, :].astype(F32) * b
                    col = (k * heads + j) * 128
                    all_s[p * rows : (p + 1) * rows, col : col + 128] = jnp.transpose(o.astype(BF16))

    acc = jnp.dot(all_s[:, 0:part], w_own[...], preferred_element_type=F32)
    acc = acc + jnp.dot(all_s[:, part : 2 * part], w_oth[...], preferred_element_type=F32)
    for p in range(prompts):
        y = hidden[p].astype(F32) + gate[p] * acc[p * rows : (p + 1) * rows, :]
        out[p] = (y + cached[p].astype(F32)).astype(BF16)


def project(info, got, near, far, w_out, w_oth, gate, hidden, cached):
    prompts, rows, width = hidden.shape
    part = w_out.shape[0]
    bn = 768
    steps = width // bn
    return pl.pallas_call(
        project_body,
        grid_spec=pltpu.PrefetchScalarGridSpec(
            num_scalar_prefetch=1,
            grid=(steps,),
            in_specs=[
                pl.BlockSpec(got.shape, lambda n, s: (0, 0, 0)),
                pl.BlockSpec(near.shape, lambda n, s: (0, 0, 0, 0)),
                pl.BlockSpec(far.shape, lambda n, s: (0, 0, 0, 0)),
                pl.BlockSpec((part, bn), lambda n, s: (0, s[0] * steps + n)),
                pl.BlockSpec((part, bn), lambda n, s: (0, n)),
                pl.BlockSpec((prompts, 1, bn), lambda n, s: (0, 0, n)),
                pl.BlockSpec((prompts, rows, bn), lambda n, s: (0, 0, n)),
                pl.BlockSpec((prompts, rows, bn), lambda n, s: (0, 0, n)),
            ],
            out_specs=pl.BlockSpec((prompts, rows, bn), lambda n, s: (0, 0, n)),
            scratch_shapes=[pltpu.VMEM((prompts * rows, 2 * part), BF16)],
        ),
        out_shape=jax.ShapeDtypeStruct((prompts, rows, width), BF16),
        compiler_params=pltpu.CompilerParams(
            dimension_semantics=("arbitrary",), vmem_limit_bytes=VMEM
        ),
        cost_estimate=pl.CostEstimate(
            flops=4 * prompts * rows * part * width, bytes_accessed=12_000_000, transcendentals=0
        ),
        name="project",
    )(info, got, near, far, w_out, w_oth, gate, hidden, cached)


def per_device(
    image_hidden,
    modulation,
    qkv_weight,
    out_weight,
    q_gain,
    k_gain,
    text_keys,
    text_values,
    stale_keys,
    stale_values,
    cached_residual,
    patch_of,
    refresh,
    text_len,
):
    prompts, rows, width_part = image_hidden.shape
    head_dim = q_gain.shape[0]
    channels = out_weight.shape[0]
    heads = channels // head_dim
    seat = lax.axis_index("seq")
    head_seat = lax.axis_index("head")
    batch_seat = lax.axis_index("batch")
    n_seq = lax.axis_size("seq")
    n_batch = lax.axis_size("batch")
    swap = [(0, 1), (1, 0)]

    halves = 2
    half = rows // halves
    other_hidden = []
    for i in range(halves):
        other_hidden.append(lax.ppermute(image_hidden[:, i * half : (i + 1) * half], "head", swap))

    text = jnp.stack([text_keys, text_values], 1)
    t_rows = text.shape[2]
    text = text.reshape(prompts, 2, t_rows, heads, head_dim).transpose(0, 3, 1, 2, 4)
    text = jnp.pad(text, ((0, 0), (0, SLOTS - heads), (0, 0), (0, 0), (0, 0)))
    text = text.reshape(n_seq, 2, t_rows, head_dim)
    text = lax.all_to_all(text, "seq", split_axis=0, concat_axis=0, tiled=True)
    text_k = text[:, 0].reshape(n_seq * t_rows, head_dim)
    text_v = text[:, 1].reshape(n_seq * t_rows, head_dim).T

    n_y = n_seq // 4
    y_seat = seat // 4
    share = channels // (n_batch * n_y)
    piece = lax.dynamic_slice(
        out_weight,
        ((batch_seat * n_y + y_seat) * share, (1 - head_seat) * width_part),
        (share, width_part),
    )
    piece = lax.ppermute(piece, "head", swap)

    seats = jnp.arange(n_seq, dtype=jnp.int32)
    own_band = jnp.sum(jnp.where(seats == seat, patch_of, 0))
    own_flag = jnp.sum(jnp.where(seats == seat, refresh, 0))
    raster = own_band * rows + jnp.arange(rows, dtype=jnp.int32)
    cos, sin = rotary_tables(raster, head_dim, GRID_W)
    info = jnp.stack([head_seat.astype(jnp.int32), own_flag.astype(jnp.int32)])
    mod_view = modulation.transpose(1, 0, 2)
    weight_view = qkv_weight.transpose(1, 0, 2)
    gains = jnp.stack([q_gain, k_gain])
    send, fresh, got = [], [], []
    for i in range(halves):
        s, f = qkv(
            i,
            info,
            image_hidden,
            other_hidden[i],
            mod_view,
            weight_view,
            gains,
            cos,
            sin,
            stale_keys,
            stale_values,
        )
        send.append(s)
        fresh.append(f)
        got.append(
            lax.all_to_all(
                s.reshape(n_seq, 3, half, head_dim), "seq", split_axis=0, concat_axis=0, tiled=True
            )
        )
    piece, _ = lax.optimization_barrier((piece, send[0]))
    w_y = jnp.zeros((n_y, share, width_part), BF16)
    w_y = lax.dynamic_update_slice(w_y, piece[None], (y_seat, 0, 0))
    for d in range(1, n_y):
        moved = lax.ppermute(piece, "seq", [(i, (i + 4 * d) % n_seq) for i in range(n_seq)])
        w_y = lax.dynamic_update_slice(w_y, moved[None], ((y_seat - d) % n_y, 0, 0))
    w_y, _ = lax.optimization_barrier((w_y, send[1]))
    w_oth = jnp.zeros((n_batch, n_y, share, width_part), BF16)
    w_oth = lax.dynamic_update_slice(w_oth, w_y[None], (batch_seat, 0, 0, 0))
    for d in range(1, n_batch):
        moved = lax.ppermute(w_y, "batch", [(i, (i + d) % n_batch) for i in range(n_batch)])
        w_oth = lax.dynamic_update_slice(w_oth, moved[None], ((batch_seat - d) % n_batch, 0, 0, 0))
    w_oth = w_oth.reshape(channels, width_part)
    near = diag(send, fresh)
    got[1], near_sent = lax.optimization_barrier((got[1], near))
    far = lax.ppermute(near_sent, "head", swap)
    unit_prompt = jnp.minimum(seat // SLOTS, prompts - 1)
    length = jnp.sum(jnp.where(jnp.arange(prompts) == unit_prompt, text_len, 0)).astype(jnp.int32)
    back = attend(length[None], got, text_k, text_v)
    back = lax.all_to_all(
        back.reshape(n_seq * 2, 144, rows), ("seq", "head"), split_axis=0, concat_axis=0, tiled=True
    )
    gate = lax.dynamic_slice_in_dim(modulation[:, 2:3], head_seat * width_part, width_part, 2)
    return project(info, back, near, far, out_weight, w_oth, gate, image_hidden, cached_residual)


def solution(mesh):
    in_specs = (
        P("batch", "seq", "head"),
        P("batch", None, None),
        P(None, None, "head"),
        P("head", None),
        P(),
        P(),
        P("batch", "seq", "head"),
        P("batch", "seq", "head"),
        P("batch", "seq", "head"),
        P("batch", "seq", "head"),
        P("batch", "seq", "head"),
        P("batch"),
        P("batch"),
        P("batch"),
    )
    out_specs = P("batch", "seq", "head")
    return jax.shard_map(
        per_device, mesh=mesh, in_specs=in_specs, out_specs=out_specs, check_vma=False
    )
```
